32 devices in a mesh: vol: 8 (over z, y), pix: 4 (over x, core).
Axes of the slice: x: 2, y: 2, z: 4, core: 2. Of those that a mesh axis runs over, the one named last changes fastest.
Arguments:
- kernel: bfloat16 [524288, 128], P(('vol', 'pix')), may hold values from 0 to 0.25
- pressure: bfloat16 [524288], P(('vol', 'pix')), may hold values from 0.049804688 to 2
- velocity: bfloat16 [524288], P(('vol', 'pix')), may hold values from -4 to 4
- entry_slot: int32 [32, 16384], P(('vol', 'pix')), may hold values from 0 to 1023, never falling along the last dimension, each value on 1 to 32 neighbouring positions
- slot_tile: int32 [32, 1024], P(('vol', 'pix')), may hold values from 0 to 8191, as said below
- tile_owner: int32 [8192], replicated, may hold values from 0 to 3, as said below
Outputs:
- owned_tiles: float32 [16384, 256], P(('vol', 'pix'))
- shell_map: float32 [8192, 256], P('vol')
The draws below stay inside these ranges and needn't reach their ends.
Inputs may be any that keep to these rules, and one draw needn't show every extreme that they name: `entry_slot`: for each device the slot numbers never fall along its 16384 crossings; every slot has at least one crossing and at most 32. `tile_owner`: within every block of 1024 consecutive tiles each pix index owns 256 // 2 to 512 tiles, and one owner of each block owns exactly 512. `slot_tile`: the 1024 tiles of one device are distinct; at most 64 of them belong to any one owning device (vol index t // 1024, pix index tile_owner[t]), and one owning device gets exactly 64 from every device.
All inputs are finite; a program needn't handle non-finite values.
Results may differ from the reference program's by a relative error of at most 0.0003.
Values sent between devices are 32-bit elements; how exact they have to be, the bound alone decides.
A program may use at most 64 MiB of HBM per device.

```python
import math
import jax
import jax.numpy as jnp
import numpy as np
from jax import lax

PIX_TILE = 128
CHANNELS = 2
ENTRIES = 16384
SLOTS = 1024
TILE_DEV = 256
TILE_V = 1024
TILES = 8192
OWN_MAX = 512
CAP = 64
N_VOL = 8
N_PIX = 4
DEVICES = 32


def ownership(key):
    groups = TILE_V // TILE_DEV
    vol_count = TILES // TILE_V
    least_owned = TILE_DEV // 2
    most_owned = 2 * TILE_DEV
    remainder = TILE_V - most_owned - (groups - 1) * least_owned
    labels = jnp.arange(groups, dtype=jnp.int32)

    def one_block(block_key):
        busiest_key, pool_key, mix_key = jax.random.split(block_key, 3)
        busiest = jax.random.randint(busiest_key, (), 0, groups, dtype=jnp.int32)
        baseline = jnp.repeat(labels, least_owned)
        extra_top = jnp.full((most_owned - least_owned,), 1, jnp.int32) * busiest
        token_pool = jax.random.permutation(pool_key, jnp.repeat(labels, most_owned - least_owned))
        ordering = jnp.argsort((token_pool == busiest).astype(jnp.int32), stable=True)
        chosen = token_pool[ordering][:remainder]
        block_owner = jnp.concatenate([baseline, extra_top, chosen]).astype(jnp.int32)
        return (jax.random.permutation(mix_key, block_owner), busiest)
    owners, busiest_overall = jax.vmap(one_block)(jax.random.split(key, vol_count))
    heavy_vol = jax.random.randint(jax.random.fold_in(key, 7), (), 0, vol_count, dtype=jnp.int32)
    heavy_device = heavy_vol * groups + busiest_overall[heavy_vol]
    return (owners.astype(jnp.int32), heavy_device.astype(jnp.int32))


def draw_tile_owner(key, part):
    owners, heavy_device = ownership(jax.random.fold_in(key, 101))
    return owners.reshape(TILES)


def draw_slot_tile(key, part):
    owners, heavy_device = ownership(jax.random.fold_in(key, 101))
    groups = TILE_V // TILE_DEV
    vol_count = TILES // TILE_V
    device_count = vol_count * groups
    flat_owner = owners.reshape(TILES)
    holder = jnp.arange(TILES, dtype=jnp.int32) // TILE_V * groups + flat_owner
    held_count = jax.ops.segment_sum(jnp.ones((TILES,), jnp.int32), holder, num_segments=device_count)
    first_row = (jnp.cumsum(held_count, dtype=jnp.int32) - held_count).astype(jnp.int32)
    labels = jnp.arange(device_count, dtype=jnp.int32)

    def one_device(device_key):
        pool_key, ranking_random_key, mix_key = jax.random.split(device_key, 3)
        token_pool = jax.random.permutation(pool_key, jnp.repeat(labels, CAP))
        ordering = jnp.argsort((token_pool == heavy_device).astype(jnp.int32), stable=True)
        chosen = token_pool[ordering][:SLOTS - CAP]
        wanted = jax.ops.segment_sum(jnp.ones((SLOTS - CAP,), jnp.int32), chosen, num_segments=device_count)
        wanted = wanted + CAP * (labels == heavy_device).astype(jnp.int32)
        shuffle = jax.random.permutation(ranking_random_key, TILES).astype(jnp.int32)
        grouped = jnp.argsort(holder * TILES + shuffle, stable=True).astype(jnp.int32)
        position = jnp.arange(TILES, dtype=jnp.int32) - first_row[holder[grouped]]
        selected = position < wanted[holder[grouped]]
        positions = jnp.nonzero(selected, size=SLOTS)[0]
        tile_ids = grouped[positions].astype(jnp.int32)
        return jax.random.permutation(mix_key, tile_ids)
    device_keys = jax.random.split(jax.random.fold_in(key, 202), device_count)
    return jax.vmap(one_device)(device_keys).astype(jnp.int32)


def levels(rng, dims, cuts, low, high):
    def one(axis_at, blocks):
        heights = jax.random.uniform(jax.random.fold_in(jax.random.fold_in(rng, 6), axis_at), (blocks,), jnp.float32, low / len(cuts), high / len(cuts))
        return jnp.repeat(jnp.exp(heights), dims[axis_at] // blocks).reshape((-1,) + (1,) * (len(dims) - axis_at - 1))

    factor_of = one(*cuts[0])
    for cut in cuts[1:]:
        factor_of = factor_of * one(*cut)
    return factor_of


def profile(number_of, total, limit, skew):
    loads = [(1 << 20) // math.isqrt(rank ** skew) + 1 for rank in range(2, number_of + 1)]
    spare, counts = total - limit - (number_of - 1), [1] * (number_of - 1)
    while spare > 0:
        candidates = [i for i in range(number_of - 1) if counts[i] < limit]
        pool, left = sum([loads[i] for i in candidates]), spare
        for i in candidates:
            more = min(limit - counts[i], max(1, left * loads[i] // pool), spare)
            counts[i] = counts[i] + more
            spare = spare - more
    return np.array([limit] + counts)


def ragged(stream_key, number_of, total, limit, slope):
    if number_of == 2:
        one = jax.random.randint(stream_key, (), max(1, total - limit), min(limit, total - 1) + 1)
        return jnp.stack([one, total - one])
    tallies = jnp.asarray(profile(number_of, total, limit, slope), jnp.int32)
    twos = (number_of - 1) // 2
    donor, receiver = tallies[1:1 + 2 * twos:2], tallies[2:2 + 2 * twos:2]
    margin = jnp.minimum(donor - 1, limit - receiver)
    passed = jax.random.randint(jax.random.fold_in(stream_key, 1), (twos,), 0, 1 << 20) % (margin + 1)
    tallies = tallies.at[1:1 + 2 * twos:2].set(donor - passed).at[2:2 + 2 * twos:2].set(receiver + passed)
    return tallies[jax.random.permutation(jax.random.fold_in(stream_key, 2), number_of)]


def normal_values(rng, shape, spread, reach, shards=(), kind=jnp.bfloat16):
    loudness = levels(rng, shape, shards, -0.22, 0.18) if shards else 1.0
    values = jax.random.normal(rng, shape, jnp.float32) * spread * loudness
    return jnp.minimum(jnp.maximum(values, -reach), reach).astype(kind)


def setup_inputs(seed: int = 0) -> dict:
    splits = jax.random.split(jax.random.key(seed), 7)
    return {
        "kernel": jnp.clip(0.25 * jax.random.uniform(splits[0], (DEVICES * ENTRIES, PIX_TILE), jnp.float32) ** levels(splits[0], (DEVICES * ENTRIES, PIX_TILE), ((0, 32),), -0.2, 0.2), 0.0, 0.25).astype(jnp.bfloat16),
        "pressure": jnp.clip(jnp.exp(math.log(2.0) - 3.6927934 * jax.random.uniform(splits[1], (DEVICES * ENTRIES,), jnp.float32) ** levels(splits[1], (DEVICES * ENTRIES,), ((0, 32),), -0.2, 0.2)), 0.049804688, 2.0).astype(jnp.bfloat16),
        "velocity": normal_values(splits[2], (DEVICES * ENTRIES,), 1.0, 4.0, ((0, 32),)),
        "entry_slot": jax.vmap(lambda own: jnp.searchsorted(jnp.cumsum(ragged(own, SLOTS, ENTRIES, 2 * ENTRIES // SLOTS, 1)), jnp.arange(ENTRIES), side="right"))(jax.random.split(splits[3], DEVICES)).reshape((DEVICES, ENTRIES)).astype(jnp.int32),
        "slot_tile": draw_slot_tile(jax.random.fold_in(splits[6], 71), 0),
        "tile_owner": draw_tile_owner(jax.random.fold_in(splits[6], 71), 0),
    }


def reference(kernel, pressure, velocity, entry_slot, slot_tile, tile_owner):
    kernel_weights = kernel.reshape(DEVICES, ENTRIES, PIX_TILE)
    amplitude = jnp.stack([pressure, velocity], axis=-1).reshape(DEVICES, ENTRIES, CHANNELS)

    def accumulate(running, inputs):
        device_kernel, device_amplitude, device_slot, device_tile = inputs
        pixel_products = device_amplitude.astype(jnp.float32)[:, :, None] * device_kernel.astype(jnp.float32)[:, None, :]
        partial_value = jax.ops.segment_sum(pixel_products.reshape(ENTRIES, CHANNELS * PIX_TILE), device_slot, num_segments=SLOTS)
        return running.at[device_tile].add(partial_value), None

    start_value = jnp.zeros((TILES, CHANNELS * PIX_TILE), jnp.float32)
    shell_map, unused = lax.scan(accumulate, start_value, (kernel_weights, amplitude, entry_slot, slot_tile))
    owners = tile_owner.reshape(N_VOL, TILE_V)
    matches = owners[:, None, :] == jnp.arange(N_PIX, dtype=jnp.int32)[None, :, None]
    owner_ranking = jnp.cumsum(matches.astype(jnp.int32), axis=2, dtype=jnp.int32) - 1
    owner_rank = jnp.sum(jnp.where(matches, owner_ranking, 0), axis=1, dtype=jnp.int32)
    vol_ids = jnp.arange(N_VOL, dtype=jnp.int32)[:, None]
    destination = ((vol_ids * N_PIX + owners) * OWN_MAX + owner_rank).astype(jnp.int32)
    owned_tiles = jnp.zeros((DEVICES * OWN_MAX, CHANNELS * PIX_TILE), jnp.float32)
    owned_tiles = owned_tiles.at[destination.reshape(TILES)].set(shell_map)
    return owned_tiles, shell_map
```

```python
import functools

import jax
import jax.numpy as jnp
from jax import lax
from jax.experimental import pallas as pl
from jax.experimental.pallas import tpu as pltpu
from jax.sharding import PartitionSpec as P

MESH = pl.DeviceIdType.MESH
LANES = 128
BLOCK = 256
WINDOW = 48
F32 = jnp.float32
BF16 = jnp.bfloat16
I32 = jnp.int32
PREPARE_VMEM = 24 << 20
EXCHANGE_VMEM = 24 << 20
FINISH_VMEM = 16 << 20


def iota(shape, axis):
    return lax.broadcasted_iota(I32, shape, axis)


def onehot(mask):
    return jnp.where(mask, 1.0, 0.0).astype(BF16)


def dot(a, b):
    return jnp.dot(a, b, preferred_element_type=F32)


def halves(x):
    high = x.astype(BF16)
    low = (x - high.astype(F32)).astype(BF16)
    return jnp.concatenate([high, low], axis=1)


def prepare(
    dims, kern_hbm, thermal_hbm, kinetic_hbm, slot_hbm, tile_hbm, owner_hbm,
    out_ref, rank_ref, kern_ref, slot_smem, thermal_ref, kinetic_ref, slot_ref, tile_ref, owner_ref,
    thermal32, kinetic32, part_ref, split_ref, sems, small_sem,
):
    vol_count, pix_count, slots, block_tiles, bucket = dims
    entries = kern_ref.shape[0]
    blocks = entries // BLOCK
    pieces = sems.shape[0]
    piece = entries // pieces
    lines = BLOCK // LANES

    block_high = block_tiles // LANES
    first_high = pl.multiple_of(lax.axis_index("vol") * block_high, block_high)
    small = [
        pltpu.make_async_copy(tile_hbm, tile_ref, small_sem.at[0]),
        pltpu.make_async_copy(owner_hbm.at[pl.ds(first_high, block_high)], owner_ref, small_sem.at[1]),
        pltpu.make_async_copy(slot_hbm, slot_smem, small_sem.at[2]),
        pltpu.make_async_copy(slot_hbm, slot_ref, small_sem.at[3]),
        pltpu.make_async_copy(thermal_hbm, thermal_ref, small_sem.at[4]),
        pltpu.make_async_copy(kinetic_hbm, kinetic_ref, small_sem.at[5]),
    ]
    for copy in small:
        copy.start()

    def fetch(q):
        rows = pl.ds(q * piece, piece)
        return pltpu.make_async_copy(kern_hbm.at[rows], kern_ref.at[rows], sems.at[q])

    for q in range(pieces):
        fetch(q).start()

    small[0].wait()
    small[1].wait()
    mine = owner_ref[...] == lax.axis_index("pix")
    ones = jnp.where(mine, 1.0, 0.0)
    upper = onehot(iota((LANES, LANES), 0) < iota((LANES, LANES), 1))
    above = onehot(iota((block_high, block_high), 1) < iota((block_high, block_high), 0))
    total = jnp.broadcast_to(jnp.sum(ones, axis=1, keepdims=True), (block_high, LANES))
    rank = dot(ones.astype(BF16), upper) + dot(above, total.astype(BF16))
    rank_ref[...] = jnp.where(mine, rank, -1.0).astype(I32)

    tile = tile_ref[...]
    block, low = tile // block_tiles, tile % block_tiles
    to_block = iota((vol_count, slots), 0) == block
    ones = jnp.where(to_block, 1.0, 0.0)
    carry = jnp.zeros((vol_count, 1), F32)
    position = []
    for j in range(slots // LANES):
        chunk = ones[:, j * LANES:(j + 1) * LANES]
        ranks = dot(chunk.astype(BF16), upper) + carry
        position.append(jnp.sum(chunk * ranks, axis=0, keepdims=True))
        carry = carry + jnp.sum(chunk, axis=1, keepdims=True)
    position = jnp.concatenate(position, axis=1).astype(I32)
    place = block * bucket + position

    places = onehot(iota((bucket, slots), 0) == position)
    row_high, row_low = (low // 256).astype(F32), (low % 256 + 1).astype(F32)
    values = jnp.concatenate(
        [jnp.where(to_block, row_high, 0.0), jnp.where(to_block, row_low, 0.0)], axis=0
    )
    placed = lax.dot_general(
        values.astype(BF16), places, (((1,), (1,)), ((), ())), preferred_element_type=F32
    )
    rows = placed[:vol_count] * 256.0 + placed[vol_count:] - 1.0
    for b in range(vol_count):
        names = [rows[b:b + 1, q * LANES:(q + 1) * LANES] for q in range(bucket // LANES)]
        names = jnp.concatenate(names + [jnp.zeros((8 - len(names), LANES), F32)], axis=0)
        for c in range(2):
            out_ref[b, c, bucket:bucket + 8, :] = names

    part_ref[...] = jnp.zeros_like(part_ref)
    within = iota((WINDOW, BLOCK), 0)
    for copy in small[2:]:
        copy.wait()
    thermal32[...] = thermal_ref[...].astype(F32)
    kinetic32[...] = kinetic_ref[...].astype(F32)

    def base_of(i):
        return slot_smem[lines * i, 0] // 8 * 8

    def add_window(i, base):
        def pair(ref):
            return jnp.concatenate([ref[pl.ds(lines * i + j, 1), :] for j in range(lines)], axis=1)

        base = pl.multiple_of(base, 8)
        match = within + base == pair(slot_ref)
        weights = jnp.concatenate(
            [jnp.where(match, pair(thermal32), 0.0), jnp.where(match, pair(kinetic32), 0.0)], axis=0
        ).astype(BF16)
        sums = dot(weights, kern_ref[pl.ds(pl.multiple_of(i * BLOCK, BLOCK), BLOCK), :])
        part_ref[pl.ds(base, WINDOW), 0:LANES] += sums[:WINDOW]
        part_ref[pl.ds(base, WINDOW), LANES:2 * LANES] += sums[WINDOW:]

    per = blocks // pieces
    for q in range(pieces):
        fetch(q).wait()

        def first_window(i, unused):
            add_window(i, base_of(i))
            return unused

        lax.fori_loop(q * per, (q + 1) * per, first_window, 0, unroll=4)

    def more_windows(i, unused):
        base = base_of(i)
        extra = (slot_smem[lines * i + lines - 1, LANES - 1] - base) // WINDOW

        def one(w, unused):
            add_window(i, base + w * WINDOW)
            return unused

        return lax.fori_loop(1, extra + 1, one, unused)

    lax.fori_loop(0, blocks, more_windows, 0)

    split_ref[...] = halves(part_ref[0:slots, :])

    def permute(b, unused):
        moved = dot(onehot(iota((bucket, slots), 0) + b * bucket == place), split_ref[...])
        for c in range(2):
            high, low = c * LANES, (c + 2) * LANES
            out_ref[b, c, 0:bucket, :] = moved[:, high:high + LANES] + moved[:, low:low + LANES]
        return unused

    lax.fori_loop(0, vol_count, permute, 0)


def exchange(
    dims, out_hbm, gathered, arrived, sums_ref, swapped, sums, crossed,
    send_sem, recv_sem, local_sem, swap_send, swap_recv, mid_send, mid_recv, own_send, own_recv,
    far_send, far_recv, pass_send, pass_recv,
):
    vol_count, pix_count, block_tiles, bucket = dims
    half = vol_count // 2
    near_count = 2 * half
    members = pix_count // 2
    share = block_tiles // members
    vol, pix = lax.axis_index("vol"), lax.axis_index("pix")
    side, place = vol // half, vol % half
    chip, core = pix // 2, pix % 2
    group, channel = chip // 2, chip % 2
    member = group * 2 + core
    across = (vol + half) % vol_count
    mine = place * 2 + channel

    def peer(k):
        return (place + k // 2) % half, (channel + k % 2) % 2

    def pix_of(other_group, other_channel, other_core):
        return (other_group * 2 + other_channel) * 2 + other_core

    barrier = pltpu.get_barrier_semaphore()

    def signal(other_vol, other_pix):
        pl.semaphore_signal(
            barrier, inc=1, device_id=(other_vol, other_pix), device_id_type=MESH
        )

    def greet_near(k, unused):
        other_place, other_channel = peer(k)
        signal(side * half + other_place, pix_of(group, other_channel, core))
        return unused

    signal(across, pix)
    for k in range(1, pix_count):
        signal(vol, (pix + k) % pix_count)
    lax.fori_loop(2, near_count, greet_near, 0)
    pl.semaphore_wait(barrier, near_count - 2 + pix_count)

    def final(stage, other_place):
        return (side * half + other_place + half * (1 - stage)) % vol_count

    def rows_copy(stage, k):
        other_place, other_channel = peer(k)
        return pltpu.make_async_remote_copy(
            src_ref=out_hbm.at[final(stage, other_place), other_channel],
            dst_ref=arrived.at[stage, mine],
            send_sem=send_sem.at[stage, k], recv_sem=recv_sem.at[stage, k],
            device_id=(side * half + other_place, pix_of(group, other_channel, core)),
            device_id_type=MESH,
        )

    def local_copy(stage):
        return pltpu.make_async_copy(
            out_hbm.at[final(stage, place), channel], arrived.at[stage, mine], local_sem.at[stage]
        )

    for stage in range(2):

        def send(k, unused):
            rows_copy(stage, k).start()
            return unused

        local_copy(stage).start()
        lax.fori_loop(1, near_count, send, 0)

    def sum_up(stage):
        target = sums_ref.at[stage]
        local_copy(stage).wait()
        target[...] = jnp.zeros((block_tiles, LANES), F32)

        def receive(i, unused):
            def one(j, unused):
                rows_copy(stage, 2 * i + j).wait_recv()
                return unused

            lax.fori_loop(jnp.where(i == 0, 1, 0), 2, one, 0)
            sender = (place + half - i) % half * 2
            names, values = [], []
            for j in range(2):
                for q in range(bucket // LANES):
                    names.append(arrived[stage, sender + j, bucket + q:bucket + q + 1, :])
                values.append(arrived[stage, sender + j, 0:bucket, :])
            names = jnp.concatenate(names, axis=1).astype(I32)
            places = onehot(iota((block_tiles, 2 * bucket), 0) == names)
            moved = dot(places, halves(jnp.concatenate(values, axis=0)))
            target[...] += moved[:, :LANES] + moved[:, LANES:]
            return unused

        lax.fori_loop(0, half, receive, 0)

    def swap_copy(stage, k):
        other = (member + k) % members
        return pltpu.make_async_remote_copy(
            src_ref=sums_ref.at[stage, pl.ds(other * share, share)],
            dst_ref=swapped.at[stage, k - 1],
            send_sem=swap_send.at[stage, k], recv_sem=swap_recv.at[stage, k],
            device_id=(vol, pix_of(other // 2, channel, other % 2)), device_id_type=MESH,
        )

    piece_count = mid_send.shape[0]
    piece_rows = share // piece_count

    def part(q):
        return pl.ds(q * piece_rows, piece_rows)

    def reduced(stage, q):
        rows = pl.ds(pl.multiple_of(member * share + q * piece_rows, piece_rows), piece_rows)
        value = sums_ref[stage, rows, :]
        for k in range(1, members):
            value = value + swapped[stage, k - 1, part(q), :]
        return value

    def mid_copy(q):
        return pltpu.make_async_remote_copy(
            src_ref=sums.at[part(q)], dst_ref=crossed.at[part(q)],
            send_sem=mid_send.at[q], recv_sem=mid_recv.at[q],
            device_id=(across, pix), device_id_type=MESH,
        )

    for stage in range(2):
        sum_up(stage)
        for k in range(1, members):
            swap_copy(stage, k).start()
        for k in range(1, members):
            swap_copy(stage, k).wait_recv()
        if stage == 0:
            for q in range(piece_count):
                sums[part(q), :] = reduced(0, q)
                mid_copy(q).start()

    sibling = (vol, pix - core + (1 - core))
    others = range(1, pix_count // 2)

    def far_copy(k, q):
        return pltpu.make_async_remote_copy(
            src_ref=gathered.at[pix, part(q)], dst_ref=gathered.at[pix, part(q)],
            send_sem=far_send.at[k, q], recv_sem=far_recv.at[k, q],
            device_id=(vol, (pix + 2 * k) % pix_count), device_id_type=MESH,
        )

    def pass_copy(k, q):
        source = (pix + pix_count - 2 * k) % pix_count
        return pltpu.make_async_remote_copy(
            src_ref=gathered.at[source, part(q)], dst_ref=gathered.at[source, part(q)],
            send_sem=pass_send.at[k, q], recv_sem=pass_recv.at[k, q],
            device_id=sibling, device_id_type=MESH,
        )

    def own_copy(q):
        return pltpu.make_async_remote_copy(
            src_ref=gathered.at[pix, part(q)], dst_ref=gathered.at[pix, part(q)],
            send_sem=own_send.at[q], recv_sem=own_recv.at[q],
            device_id=sibling, device_id_type=MESH,
        )

    def relay(q):
        for k in others:
            far_copy(k, q).wait_recv()
            pass_copy(k, q).start()

    for q in range(piece_count):
        mid_copy(q).wait_recv()
        gathered[pix, part(q), :] = reduced(1, q) + crossed[part(q), :]
        for k in others:
            far_copy(k, q).start()
        own_copy(q).start()
        if q:
            relay(q - 1)
    relay(piece_count - 1)
    for q in range(piece_count):
        own_copy(q).wait()
        mid_copy(q).wait_send()
        for k in others:
            far_copy(k, q).wait_send()
            pass_copy(k, q).wait()

    for stage in range(2):
        for k in range(1, members):
            swap_copy(stage, k).wait_send()

        def sent(k, unused):
            rows_copy(stage, k).wait_send()
            return unused

        lax.fori_loop(1, near_count, sent, 0)


def finish(gathered, rank_ref, owned_hbm, shell_hbm, split_ref, owned_ref, shell_sem, owned_sem):
    pix_count, share = gathered.shape[0], gathered.shape[1]
    owned_most = owned_ref.shape[0]
    block_tiles = rank_ref.shape[0] * LANES
    copies = []
    for p in range(pix_count):
        chip, core = p // 2, p % 2
        start, channel = (chip // 2 * 2 + core) * share, chip % 2
        copy = pltpu.make_async_copy(
            gathered.at[p],
            shell_hbm.at[pl.ds(start, share), pl.ds(channel * LANES, LANES)],
            shell_sem.at[p],
        )
        copy.start()
        copies.append(copy)
        both = halves(gathered[p])
        for part in range(2):
            first = (2 * part + channel) * LANES
            split_ref[start:start + share, first:first + LANES] = both[:, part * LANES:(part + 1) * LANES]
    rank = jnp.concatenate([rank_ref[q:q + 1, :] for q in range(rank_ref.shape[0])], axis=1)
    moved = dot(onehot(iota((owned_most, block_tiles), 0) == rank), split_ref[...])
    owned_ref[...] = moved[:, :2 * LANES] + moved[:, 2 * LANES:]
    copy = pltpu.make_async_copy(owned_ref, owned_hbm, owned_sem)
    copy.start()
    for other in copies + [copy]:
        other.wait()


def shards(kernel, pressure, velocity, entry_slot, slot_tile, tile_owner):
    vol_count, pix_count = lax.axis_size("vol"), lax.axis_size("pix")
    device_count = vol_count * pix_count
    entries = kernel.shape[0]
    slots = slot_tile.shape[1]
    tiles = tile_owner.shape[0]
    block_tiles = tiles // vol_count
    owned_most = 2 * block_tiles // pix_count
    bucket = 2 * slots // vol_count
    width = 2 * kernel.shape[1]
    vmem = pl.BlockSpec(memory_space=pltpu.VMEM)
    anywhere = pl.BlockSpec(memory_space=pl.ANY)
    hbm = pl.BlockSpec(memory_space=pltpu.HBM)
    dma = pltpu.SemaphoreType.DMA

    shape = (entries // LANES, LANES)
    outgoing, rank = pl.pallas_call(
        functools.partial(prepare, (vol_count, pix_count, slots, block_tiles, bucket)),
        out_shape=(
            jax.ShapeDtypeStruct((vol_count, 2, bucket + 8, LANES), F32),
            jax.ShapeDtypeStruct((block_tiles // LANES, LANES), I32),
        ),
        in_specs=[hbm] * 6,
        out_specs=(vmem, vmem),
        scratch_shapes=[
            pltpu.VMEM(kernel.shape, BF16),
            pltpu.SMEM(shape, I32),
            pltpu.VMEM(shape, BF16),
            pltpu.VMEM(shape, BF16),
            pltpu.VMEM(shape, I32),
            pltpu.VMEM((1, slots), I32),
            pltpu.VMEM((block_tiles // LANES, LANES), I32),
            pltpu.VMEM(shape, F32),
            pltpu.VMEM(shape, F32),
            pltpu.VMEM((slots + WINDOW, width), F32),
            pltpu.VMEM((slots, 2 * width), BF16),
            dma((4,)),
            dma((6,)),
        ],
        compiler_params=pltpu.CompilerParams(vmem_limit_bytes=PREPARE_VMEM),
        name="prepare",
    )(*[
        pltpu.with_memory_space_constraint(x, pltpu.HBM) for x in (
            kernel, pressure.reshape(shape), velocity.reshape(shape), entry_slot.reshape(shape),
            slot_tile, tile_owner.reshape(tiles // LANES, LANES),
        )
    ])

    pieces = 4
    chips = pix_count // 2
    near = vol_count
    share = block_tiles // chips
    gathered = pl.pallas_call(
        functools.partial(exchange, (vol_count, pix_count, block_tiles, bucket)),
        out_shape=jax.ShapeDtypeStruct((pix_count, share, LANES), F32),
        in_specs=[anywhere],
        out_specs=vmem,
        scratch_shapes=[
            pltpu.VMEM((2, near, bucket + 8, LANES), F32),
            pltpu.VMEM((2, block_tiles, LANES), F32),
            pltpu.VMEM((2, chips - 1, share, LANES), F32),
            pltpu.VMEM((share, LANES), F32),
            pltpu.VMEM((share, LANES), F32),
            dma((2, near)), dma((2, near)), dma((2,)), dma((2, chips)), dma((2, chips)),
            dma((pieces,)), dma((pieces,)), dma((pieces,)), dma((pieces,)),
            dma((chips, pieces)), dma((chips, pieces)), dma((chips, pieces)), dma((chips, pieces)),
        ],
        compiler_params=pltpu.CompilerParams(
            collective_id=0, has_side_effects=True, vmem_limit_bytes=EXCHANGE_VMEM
        ),
        name="exchange",
    )(outgoing)

    return pl.pallas_call(
        finish,
        out_shape=(
            jax.ShapeDtypeStruct((owned_most, width), F32),
            jax.ShapeDtypeStruct((block_tiles, width), F32),
        ),
        in_specs=[vmem, vmem],
        out_specs=(anywhere, anywhere),
        scratch_shapes=[
            pltpu.VMEM((block_tiles, 2 * width), BF16),
            pltpu.VMEM((owned_most, width), F32),
            dma((pix_count,)),
            dma,
        ],
        compiler_params=pltpu.CompilerParams(vmem_limit_bytes=FINISH_VMEM),
        name="finish",
    )(gathered, rank)


def solution(mesh):
    in_specs = (
        P(("vol", "pix"), None),
        P(("vol", "pix")),
        P(("vol", "pix")),
        P(("vol", "pix"), None),
        P(("vol", "pix"), None),
        P(),
    )
    out_specs = (P(("vol", "pix"), None), P("vol", None))
    return jax.shard_map(shards, mesh=mesh, in_specs=in_specs, out_specs=out_specs, check_vma=False)
```

```python
import functools

import jax
import jax.numpy as jnp
from jax import lax
from jax.experimental import pallas as pl
from jax.experimental.pallas import tpu as pltpu
from jax.sharding import PartitionSpec as P

MESH = pl.DeviceIdType.MESH
LANES = 128
BLOCK = 256
WINDOW = 48
F32 = jnp.float32
BF16 = jnp.bfloat16
I32 = jnp.int32
PREPARE_VMEM = 24 << 20
EXCHANGE_VMEM = 24 << 20
FINISH_VMEM = 16 << 20


def iota(shape, axis):
    return lax.broadcasted_iota(I32, shape, axis)


def onehot(mask):
    return jnp.where(mask, 1.0, 0.0).astype(BF16)


def dot(a, b):
    return jnp.dot(a, b, preferred_element_type=F32)


def halves(x):
    high = x.astype(BF16)
    low = (x - high.astype(F32)).astype(BF16)
    return jnp.concatenate([high, low], axis=1)


def prepare(
    dims, kern_hbm, thermal_hbm, kinetic_hbm, slot_hbm, tile_hbm, owner_hbm,
    out_ref, ids_ref, rank_ref, kern_ref, slot_smem, thermal_ref, kinetic_ref, slot_ref, tile_ref, owner_ref,
    thermal32, kinetic32, part_ref, split_ref, sems, small_sem,
):
    vol_count, pix_count, slots, block_tiles, bucket = dims
    entries = kern_ref.shape[0]
    blocks = entries // BLOCK
    pieces = sems.shape[0]
    piece = entries // pieces
    lines = BLOCK // LANES

    block_high = block_tiles // LANES
    first_high = pl.multiple_of(lax.axis_index("vol") * block_high, block_high)
    small = [
        pltpu.make_async_copy(tile_hbm, tile_ref, small_sem.at[0]),
        pltpu.make_async_copy(owner_hbm.at[pl.ds(first_high, block_high)], owner_ref, small_sem.at[1]),
        pltpu.make_async_copy(slot_hbm, slot_smem, small_sem.at[2]),
        pltpu.make_async_copy(slot_hbm, slot_ref, small_sem.at[3]),
        pltpu.make_async_copy(thermal_hbm, thermal_ref, small_sem.at[4]),
        pltpu.make_async_copy(kinetic_hbm, kinetic_ref, small_sem.at[5]),
    ]
    for copy in small:
        copy.start()

    def fetch(q):
        rows = pl.ds(q * piece, piece)
        return pltpu.make_async_copy(kern_hbm.at[rows], kern_ref.at[rows], sems.at[q])

    for q in range(pieces):
        fetch(q).start()

    small[0].wait()
    small[1].wait()
    mine = owner_ref[...] == lax.axis_index("pix")
    ones = jnp.where(mine, 1.0, 0.0)
    upper = onehot(iota((LANES, LANES), 0) < iota((LANES, LANES), 1))
    above = onehot(iota((block_high, block_high), 1) < iota((block_high, block_high), 0))
    total = jnp.broadcast_to(jnp.sum(ones, axis=1, keepdims=True), (block_high, LANES))
    rank = dot(ones.astype(BF16), upper) + dot(above, total.astype(BF16))
    rank_ref[...] = jnp.where(mine, rank, -1.0).astype(I32)

    half = vol_count // 2
    side = lax.axis_index("vol") // half
    tile = tile_ref[...]
    block, low = tile // block_tiles, tile % block_tiles
    order = (block + vol_count - (1 - side) * half) % vol_count
    to_block = iota((vol_count, slots), 0) == order
    ones = jnp.where(to_block, 1.0, 0.0)
    carry = jnp.zeros((vol_count, 1), F32)
    position = []
    for j in range(slots // LANES):
        chunk = ones[:, j * LANES:(j + 1) * LANES]
        ranks = dot(chunk.astype(BF16), upper) + carry
        position.append(jnp.sum(chunk * ranks, axis=0, keepdims=True))
        carry = carry + jnp.sum(chunk, axis=1, keepdims=True)
    position = jnp.concatenate(position, axis=1)
    starts = [jnp.zeros((1, 1), F32)]
    for b in range(vol_count - 1):
        starts.append(starts[-1] + carry[b:b + 1, :])
    starts = jnp.concatenate(starts, axis=0)
    place = (position + jnp.sum(ones * starts, axis=0, keepdims=True)).astype(I32)

    places = onehot(iota((bucket, slots), 0) == position.astype(I32))
    row_high, row_low = (low // 256).astype(F32), (low % 256 + 1).astype(F32)
    values = jnp.concatenate(
        [jnp.where(to_block, row_high, 0.0), jnp.where(to_block, row_low, 0.0)], axis=0
    )
    placed = lax.dot_general(
        values.astype(BF16), places, (((1,), (1,)), ((), ())), preferred_element_type=F32
    )
    rows = (placed[:vol_count] * 256.0 + placed[vol_count:] - 1.0).astype(I32)
    per_block = bucket // LANES
    names = jnp.concatenate(
        [rows[b:b + 1, q * LANES:(q + 1) * LANES] for b in range(vol_count) for q in range(per_block)],
        axis=0,
    )
    ids_ref[0:vol_count * per_block, :] = names
    on_lane = iota((vol_count, LANES), 0) == iota((vol_count, LANES), 1)
    line = jnp.sum(jnp.where(on_lane, starts, 0.0), axis=0, keepdims=True).astype(I32)
    ids_ref[vol_count * per_block:, :] = jnp.broadcast_to(line, (8, LANES))

    part_ref[...] = jnp.zeros_like(part_ref)
    within = iota((WINDOW, BLOCK), 0)
    for copy in small[2:]:
        copy.wait()
    thermal32[...] = thermal_ref[...].astype(F32)
    kinetic32[...] = kinetic_ref[...].astype(F32)

    def base_of(i):
        return slot_smem[lines * i, 0] // 8 * 8

    def add_window(i, base):
        def pair(ref):
            return jnp.concatenate([ref[pl.ds(lines * i + j, 1), :] for j in range(lines)], axis=1)

        base = pl.multiple_of(base, 8)
        match = within + base == pair(slot_ref)
        weights = jnp.concatenate(
            [jnp.where(match, pair(thermal32), 0.0), jnp.where(match, pair(kinetic32), 0.0)], axis=0
        ).astype(BF16)
        sums = dot(weights, kern_ref[pl.ds(pl.multiple_of(i * BLOCK, BLOCK), BLOCK), :])
        part_ref[pl.ds(base, WINDOW), 0:LANES] += sums[:WINDOW]
        part_ref[pl.ds(base, WINDOW), LANES:2 * LANES] += sums[WINDOW:]

    per = blocks // pieces
    for q in range(pieces):
        fetch(q).wait()

        def first_window(i, unused):
            add_window(i, base_of(i))
            return unused

        lax.fori_loop(q * per, (q + 1) * per, first_window, 0, unroll=4)

    def more_windows(i, unused):
        base = base_of(i)
        extra = (slot_smem[lines * i + lines - 1, LANES - 1] - base) // WINDOW

        def one(w, unused):
            add_window(i, base + w * WINDOW)
            return unused

        return lax.fori_loop(1, extra + 1, one, unused)

    lax.fori_loop(0, blocks, more_windows, 0)

    split_ref[...] = halves(part_ref[0:slots, :])

    cols, sub = LANES // half, bucket // half
    lane = iota((sub, LANES), 1) // cols

    def permute(q, unused):
        moved = dot(onehot(iota((bucket, slots), 0) + q * bucket == place), split_ref[...])
        for c in range(2):
            high, low = c * LANES, (c + 2) * LANES
            value = moved[:, high:high + LANES] + moved[:, low:low + LANES]
            rolled = [value] + [pltpu.roll(value, d * cols, 1) for d in range(1, half)]
            for h in range(half):
                packed = rolled[(half - h) % half][0:sub]
                for u in range(1, half):
                    packed = jnp.where(
                        lane == u, rolled[(u - h) % half][u * sub:(u + 1) * sub], packed
                    )
                out_ref[h, c, q] = packed
        return unused

    lax.fori_loop(0, half, permute, 0)


def exchange(
    dims, out_hbm, ids_hbm, gathered, arrived, ids, starts, rows_ref, acc, partial, swapped, sums,
    crossed, total, send_sem, recv_sem, ids_send, ids_recv, local_sem, start_sem, swap_send,
    swap_recv, mid_send, mid_recv, far_send, far_recv, own_sem, pass_send, pass_recv,
):
    vol_count, pix_count, block_tiles, bucket = dims
    half = vol_count // 2
    near_count = 2 * half
    chips = pix_count // 2
    members = chips
    cols, sub = LANES // half, bucket // half
    group_tiles = block_tiles // half
    share = group_tiles // members
    per_block = bucket // LANES
    vol, pix = lax.axis_index("vol"), lax.axis_index("pix")
    side, place = vol // half, vol % half
    chip, core = pix // 2, pix % 2
    group, channel = chip // 2, chip % 2
    member = group * 2 + core
    across = (vol + half) % vol_count
    mine = place * 2 + channel
    sibling = (vol, pix - core + (1 - core))

    def peer(k):
        return (place + k // 2) % half, (channel + k % 2) % 2

    def sender(k):
        return (place + half - k // 2) % half * 2 + (channel + k % 2) % 2

    def pix_of(other_group, other_channel, other_core):
        return (other_group * 2 + other_channel) * 2 + other_core

    barrier = pltpu.get_barrier_semaphore()

    def signal(other_vol, other_pix):
        pl.semaphore_signal(
            barrier, inc=1, device_id=(other_vol, other_pix), device_id_type=MESH
        )

    def greet(k, unused):
        signal(side * half + (place + k // chips) % half, (chip + k % chips) % chips * 2 + core)
        return unused

    signal(across, pix)
    for k in range(1, pix_count):
        signal(vol, (pix + k) % pix_count)
    lax.fori_loop(chips, half * chips, greet, 0)
    pl.semaphore_wait(barrier, pix_count + (half - 1) * chips)

    def target(k):
        other_place, other_channel = peer(k)
        return side * half + other_place, pix_of(group, other_channel, core)

    def rows_copy(q, k):
        other_place, other_channel = peer(k)
        return pltpu.make_async_remote_copy(
            src_ref=out_hbm.at[other_place, other_channel, q], dst_ref=arrived.at[q, mine],
            send_sem=send_sem.at[q, k], recv_sem=recv_sem.at[q, k],
            device_id=target(k), device_id_type=MESH,
        )

    def ids_copy(k):
        return pltpu.make_async_remote_copy(
            src_ref=ids_hbm, dst_ref=ids.at[mine],
            send_sem=ids_send.at[k], recv_sem=ids_recv.at[k],
            device_id=target(k), device_id_type=MESH,
        )

    def local_rows(q):
        return pltpu.make_async_copy(
            out_hbm.at[place, channel, q], arrived.at[q, mine], local_sem.at[q]
        )

    local_ids = pltpu.make_async_copy(ids_hbm, ids.at[mine], local_sem.at[half])

    def send_ids(k, unused):
        ids_copy(k).start()
        return unused

    lax.fori_loop(1, near_count, send_ids, 0)
    local_ids.start()

    def send_chunk(q, unused):
        def one(k, unused):
            rows_copy(q, k).start()
            return unused

        lax.fori_loop(1, near_count, one, 0)
        local_rows(q).start()
        return unused

    lax.fori_loop(0, half, send_chunk, 0)

    def clear(s, unused):
        rows_ref[s, half * bucket:(half + 1) * bucket, :] = jnp.zeros((bucket, LANES), F32)
        return unused

    lax.fori_loop(0, near_count, clear, 0)

    def start_copy(s):
        return pltpu.make_async_copy(
            ids.at[s, pl.ds(vol_count * per_block, 1)], starts.at[pl.ds(s, 1)], start_sem.at[s]
        )

    local_ids.wait()
    start_copy(mine).start()

    def take_ids(k, unused):
        ids_copy(k).wait_recv()
        start_copy(sender(k)).start()
        return unused

    lax.fori_loop(1, near_count, take_ids, 0)

    def take_starts(s, unused):
        start_copy(s).wait()
        return unused

    lax.fori_loop(0, near_count, take_starts, 0)

    lane = iota((1, LANES), 1) // cols
    wide = iota((sub, LANES), 1) // cols

    def unpack(q, s):
        value = arrived[q, s]
        rolled = [value] + [pltpu.roll(value, d * cols, 1) for d in range(1, half)]
        for u in range(half):
            spread = rolled[(half - u) % half]
            for v in range(1, half):
                spread = jnp.where(wide == v, rolled[(v - u) % half], spread)
            first = pl.multiple_of(q * bucket + u * sub, sub)
            rows_ref[s, pl.ds(first, sub), :] = spread

    def accumulate(b, s):
        both = halves(rows_ref[s, pl.ds(starts[s, b], bucket), :])
        names = jnp.concatenate(
            [ids[s, pl.ds(b * per_block + j, 1), :] for j in range(per_block)], axis=1
        )
        tile = iota((group_tiles, bucket), 0)
        places, values = [], []
        for u in range(half):
            places.append(onehot(tile + u * group_tiles == names))
            keep = onehot(lane == u)
            values.append(both * jnp.concatenate([keep, keep], axis=1))
        acc[...] += dot(jnp.concatenate(places, axis=1), jnp.concatenate(values, axis=0))

    def swap_copy(b, k):
        other = (member + k) % members
        return pltpu.make_async_remote_copy(
            src_ref=partial.at[b, pl.ds(other * share, share)], dst_ref=swapped.at[b, k - 1],
            send_sem=swap_send.at[b, k], recv_sem=swap_recv.at[b, k],
            device_id=(vol, pix_of(other // 2, channel, other % 2)), device_id_type=MESH,
        )

    def swap(b):
        partial[b] = acc[:, :LANES] + acc[:, LANES:]
        for k in range(1, members):
            swap_copy(b, k).start()

    def reduced(b):
        for k in range(1, members):
            swap_copy(b, k).wait_recv()
        value = partial[b, pl.ds(pl.multiple_of(member * share, share), share), :]
        for k in range(1, members):
            value = value + swapped[b, k - 1]
        return value

    def mid_copy(b):
        return pltpu.make_async_remote_copy(
            src_ref=sums.at[b], dst_ref=crossed.at[b],
            send_sem=mid_send.at[b], recv_sem=mid_recv.at[b],
            device_id=(across, pix), device_id_type=MESH,
        )

    def far(q, unused):
        acc[...] = jnp.zeros(acc.shape, F32)
        local_rows(q).wait()
        unpack(q, mine)
        accumulate(q, mine)

        def one(k, unused):
            rows_copy(q, k).wait_recv()
            unpack(q, sender(k))
            accumulate(q, sender(k))
            return unused

        lax.fori_loop(1, near_count, one, 0)
        swap(q)
        sums[q] = reduced(q)
        mid_copy(q).start()
        return unused

    lax.fori_loop(0, half, far, 0)

    def off(i):
        return (i + half - place) % half

    def far_copy(i, k):
        return pltpu.make_async_remote_copy(
            src_ref=total.at[i], dst_ref=gathered.at[core, place, chip],
            send_sem=far_send.at[off(i), k], recv_sem=far_recv.at[off(i), k],
            device_id=(side * half + i, (chip + k) % chips * 2 + core), device_id_type=MESH,
        )

    def own_copy():
        return pltpu.make_async_copy(total.at[place], gathered.at[core, place, chip], own_sem)

    def finalize(i):
        value = reduced(half + i)
        mid_copy(i).wait_recv()
        total[i] = value + crossed[i]

        @pl.when(i != place)
        def _():
            far_copy(i, 0).start()

        @pl.when(i == place)
        def _():
            own_copy().start()

        for k in range(1, chips):
            far_copy(i, k).start()

    def near(i, unused):
        acc[...] = jnp.zeros(acc.shape, F32)

        def one(s, unused):
            accumulate(half + i, s)
            return unused

        lax.fori_loop(0, near_count, one, 0)
        swap(half + i)

        @pl.when(i > 0)
        def _():
            finalize(i - 1)

        return unused

    lax.fori_loop(0, half, near, 0)
    finalize(half - 1)

    def pass_copy(o, k):
        piece = gathered.at[core, (place + half - o) % half, (chip + chips - k) % chips]
        return pltpu.make_async_remote_copy(
            src_ref=piece, dst_ref=piece,
            send_sem=pass_send.at[o, k], recv_sem=pass_recv.at[o, k],
            device_id=sibling, device_id_type=MESH,
        )

    def far_arrival(o, k):
        return pltpu.make_async_remote_copy(
            src_ref=total.at[0], dst_ref=gathered.at[core, place, chip],
            send_sem=far_send.at[o, k], recv_sem=far_recv.at[o, k],
            device_id=(side * half + (place + o) % half, (chip + k) % chips * 2 + core),
            device_id_type=MESH,
        )

    own_copy().wait()
    pass_copy(0, 0).start()
    for k in range(1, chips):
        far_arrival(0, k).wait_recv()
        pass_copy(0, k).start()

    def relay(o, unused):
        for k in range(chips):
            far_arrival(o, k).wait_recv()
            pass_copy(o, k).start()
        return unused

    lax.fori_loop(1, half, relay, 0)

    def passed(o, unused):
        for k in range(chips):
            pass_copy(o, k).wait()
        return unused

    lax.fori_loop(0, half, passed, 0)
    for k in range(1, chips):
        far_arrival(0, k).wait_send()

    def sent(o, unused):
        for k in range(chips):
            far_arrival(o, k).wait_send()
        return unused

    lax.fori_loop(1, half, sent, 0)

    def sent_rows(k, unused):
        ids_copy(k).wait_send()

        def one(q, unused):
            rows_copy(q, k).wait_send()
            return unused

        lax.fori_loop(0, half, one, 0)
        return unused

    lax.fori_loop(1, near_count, sent_rows, 0)

    def sent_sums(b, unused):
        mid_copy(b).wait_send()
        for k in range(1, members):
            swap_copy(b, k).wait_send()
            swap_copy(half + b, k).wait_send()
        return unused

    lax.fori_loop(0, half, sent_sums, 0)


def finish(
    gathered, rank_ref, owned_hbm, shell_hbm, split_ref, shell_ref, owned_ref, shell_sem, owned_sem,
):
    half, chips, share = gathered.shape[1], gathered.shape[2], gathered.shape[3]
    cols = LANES // half
    owned_most = owned_ref.shape[0]
    block_tiles = shell_ref.shape[0]
    group_tiles = block_tiles // half
    lane = iota((share, LANES), 1) // cols
    for core in range(2):
        for chip in range(chips):
            first, channel = (chip // 2 * 2 + core) * share, chip % 2
            rolled = []
            for s in range(half):
                value = gathered[core, s, chip]
                rolled.append([value] + [pltpu.roll(value, d * cols, 1) for d in range(1, half)])
            for u in range(half):
                value = rolled[0][(half - u) % half]
                for s in range(1, half):
                    value = jnp.where(lane == s, rolled[s][(s - u) % half], value)
                start = u * group_tiles + first
                shell_ref[start:start + share, channel * LANES:(channel + 1) * LANES] = value
                both = halves(value)
                for part in range(2):
                    at = (2 * part + channel) * LANES
                    split_ref[start:start + share, at:at + LANES] = both[:, part * LANES:(part + 1) * LANES]
    shell_copy = pltpu.make_async_copy(shell_ref, shell_hbm, shell_sem)
    shell_copy.start()
    rank = jnp.concatenate([rank_ref[q:q + 1, :] for q in range(rank_ref.shape[0])], axis=1)
    moved = dot(onehot(iota((owned_most, block_tiles), 0) == rank), split_ref[...])
    owned_ref[...] = moved[:, :2 * LANES] + moved[:, 2 * LANES:]
    owned_copy = pltpu.make_async_copy(owned_ref, owned_hbm, owned_sem)
    owned_copy.start()
    shell_copy.wait()
    owned_copy.wait()


def shards(kernel, pressure, velocity, entry_slot, slot_tile, tile_owner):
    vol_count, pix_count = lax.axis_size("vol"), lax.axis_size("pix")
    device_count = vol_count * pix_count
    entries = kernel.shape[0]
    slots = slot_tile.shape[1]
    tiles = tile_owner.shape[0]
    block_tiles = tiles // vol_count
    owned_most = 2 * block_tiles // pix_count
    bucket = 2 * slots // vol_count
    width = 2 * kernel.shape[1]
    vmem = pl.BlockSpec(memory_space=pltpu.VMEM)
    anywhere = pl.BlockSpec(memory_space=pl.ANY)
    hbm = pl.BlockSpec(memory_space=pltpu.HBM)
    dma = pltpu.SemaphoreType.DMA

    shape = (entries // LANES, LANES)
    half = vol_count // 2
    sub = bucket // half
    id_rows = vol_count * bucket // LANES + 8
    outgoing, ids, rank = pl.pallas_call(
        functools.partial(prepare, (vol_count, pix_count, slots, block_tiles, bucket)),
        out_shape=(
            jax.ShapeDtypeStruct((half, 2, half, sub, LANES), F32),
            jax.ShapeDtypeStruct((id_rows, LANES), I32),
            jax.ShapeDtypeStruct((block_tiles // LANES, LANES), I32),
        ),
        in_specs=[hbm] * 6,
        out_specs=(vmem, vmem, vmem),
        scratch_shapes=[
            pltpu.VMEM(kernel.shape, BF16),
            pltpu.SMEM(shape, I32),
            pltpu.VMEM(shape, BF16),
            pltpu.VMEM(shape, BF16),
            pltpu.VMEM(shape, I32),
            pltpu.VMEM((1, slots), I32),
            pltpu.VMEM((block_tiles // LANES, LANES), I32),
            pltpu.VMEM(shape, F32),
            pltpu.VMEM(shape, F32),
            pltpu.VMEM((slots + WINDOW, width), F32),
            pltpu.VMEM((slots, 2 * width), BF16),
            dma((4,)),
            dma((6,)),
        ],
        compiler_params=pltpu.CompilerParams(vmem_limit_bytes=PREPARE_VMEM),
        name="prepare",
    )(*[
        pltpu.with_memory_space_constraint(x, pltpu.HBM) for x in (
            kernel, pressure.reshape(shape), velocity.reshape(shape), entry_slot.reshape(shape),
            slot_tile, tile_owner.reshape(tiles // LANES, LANES),
        )
    ])

    chips = pix_count // 2
    near = vol_count
    group_tiles = block_tiles // half
    share = group_tiles // chips
    gathered = pl.pallas_call(
        functools.partial(exchange, (vol_count, pix_count, block_tiles, bucket)),
        out_shape=jax.ShapeDtypeStruct((2, half, chips, share, LANES), F32),
        in_specs=[anywhere, anywhere],
        out_specs=vmem,
        scratch_shapes=[
            pltpu.VMEM((half, near, sub, LANES), F32),
            pltpu.VMEM((near, id_rows, LANES), I32),
            pltpu.SMEM((near, LANES), I32),
            pltpu.VMEM((near, (half + 1) * bucket, LANES), F32),
            pltpu.VMEM((group_tiles, 2 * LANES), F32),
            pltpu.VMEM((vol_count, group_tiles, LANES), F32),
            pltpu.VMEM((vol_count, chips - 1, share, LANES), F32),
            pltpu.VMEM((half, share, LANES), F32),
            pltpu.VMEM((half, share, LANES), F32),
            pltpu.VMEM((half, share, LANES), F32),
            dma((half, near)), dma((half, near)), dma((near,)), dma((near,)),
            dma((half + 1,)), dma((near,)), dma((vol_count, chips)), dma((vol_count, chips)),
            dma((half,)), dma((half,)), dma((half, chips)), dma((half, chips)), dma,
            dma((half, chips)), dma((half, chips)),
        ],
        compiler_params=pltpu.CompilerParams(
            collective_id=0, has_side_effects=True, vmem_limit_bytes=EXCHANGE_VMEM
        ),
        name="exchange",
    )(outgoing, ids)

    return pl.pallas_call(
        finish,
        out_shape=(
            jax.ShapeDtypeStruct((owned_most, width), F32),
            jax.ShapeDtypeStruct((block_tiles, width), F32),
        ),
        in_specs=[vmem, vmem],
        out_specs=(anywhere, anywhere),
        scratch_shapes=[
            pltpu.VMEM((block_tiles, 2 * width), BF16),
            pltpu.VMEM((block_tiles, width), F32),
            pltpu.VMEM((owned_most, width), F32),
            dma,
            dma,
        ],
        compiler_params=pltpu.CompilerParams(vmem_limit_bytes=FINISH_VMEM),
        name="finish",
    )(gathered, rank)


def solution(mesh):
    in_specs = (
        P(("vol", "pix"), None),
        P(("vol", "pix")),
        P(("vol", "pix")),
        P(("vol", "pix"), None),
        P(("vol", "pix"), None),
        P(),
    )
    out_specs = (P(("vol", "pix"), None), P("vol", None))
    return jax.shard_map(shards, mesh=mesh, in_specs=in_specs, out_specs=out_specs, check_vma=False)
```

```python
import functools

import jax
import jax.numpy as jnp
from jax import lax
from jax.experimental import pallas as pl
from jax.experimental.pallas import tpu as pltpu
from jax.sharding import PartitionSpec as P

MESH = pl.DeviceIdType.MESH
LANES = 128
BLOCK = 256
WINDOW = 48
F32 = jnp.float32
BF16 = jnp.bfloat16
I32 = jnp.int32
PREPARE_VMEM = 24 << 20
EXCHANGE_VMEM = 24 << 20
FINISH_VMEM = 16 << 20


def iota(shape, axis):
    return lax.broadcasted_iota(I32, shape, axis)


def onehot(mask):
    return jnp.where(mask, 1.0, 0.0).astype(BF16)


def dot(a, b):
    return jnp.dot(a, b, preferred_element_type=F32)


def halves(x):
    high = x.astype(BF16)
    low = (x - high.astype(F32)).astype(BF16)
    return jnp.concatenate([high, low], axis=1)


def prepare(
    dims, kern_hbm, thermal_hbm, kinetic_hbm, slot_hbm, tile_hbm, owner_hbm,
    out_ref, ids_ref, rank_ref, kern_ref, slot_smem, thermal_ref, kinetic_ref, slot_ref, tile_ref, owner_ref,
    thermal32, kinetic32, part_ref, split_ref, sems, small_sem,
):
    vol_count, pix_count, slots, block_tiles, bucket = dims
    entries = kern_ref.shape[0]
    blocks = entries // BLOCK
    pieces = sems.shape[0]
    piece = entries // pieces
    lines = BLOCK // LANES

    block_high = block_tiles // LANES
    first_high = pl.multiple_of(lax.axis_index("vol") * block_high, block_high)
    small = [
        pltpu.make_async_copy(tile_hbm, tile_ref, small_sem.at[0]),
        pltpu.make_async_copy(owner_hbm.at[pl.ds(first_high, block_high)], owner_ref, small_sem.at[1]),
        pltpu.make_async_copy(slot_hbm, slot_smem, small_sem.at[2]),
        pltpu.make_async_copy(slot_hbm, slot_ref, small_sem.at[3]),
        pltpu.make_async_copy(thermal_hbm, thermal_ref, small_sem.at[4]),
        pltpu.make_async_copy(kinetic_hbm, kinetic_ref, small_sem.at[5]),
    ]
    for copy in small:
        copy.start()

    def fetch(q):
        rows = pl.ds(q * piece, piece)
        return pltpu.make_async_copy(kern_hbm.at[rows], kern_ref.at[rows], sems.at[q])

    for q in range(pieces):
        fetch(q).start()

    small[0].wait()
    small[1].wait()
    mine = owner_ref[...] == lax.axis_index("pix")
    ones = jnp.where(mine, 1.0, 0.0)
    upper = onehot(iota((LANES, LANES), 0) < iota((LANES, LANES), 1))
    above = onehot(iota((block_high, block_high), 1) < iota((block_high, block_high), 0))
    total = jnp.broadcast_to(jnp.sum(ones, axis=1, keepdims=True), (block_high, LANES))
    rank = dot(ones.astype(BF16), upper) + dot(above, total.astype(BF16))
    rank_ref[...] = jnp.where(mine, rank, -1.0).astype(I32)

    half = vol_count // 2
    side = lax.axis_index("vol") // half
    tile = tile_ref[...]
    block, low = tile // block_tiles, tile % block_tiles
    order = (block + vol_count - (1 - side) * half) % vol_count
    group_tiles = block_tiles // half
    kinds = vol_count * half
    to_kind = iota((kinds, slots), 0) == order * half + low // group_tiles
    ones = jnp.where(to_kind, 1.0, 0.0)
    carry = jnp.zeros((kinds, 1), F32)
    position = []
    for j in range(slots // LANES):
        chunk = ones[:, j * LANES:(j + 1) * LANES]
        ranks = dot(chunk.astype(BF16), upper) + carry
        position.append(jnp.sum(chunk * ranks, axis=0, keepdims=True))
        carry = carry + jnp.sum(chunk, axis=1, keepdims=True)
    counts = jnp.broadcast_to(carry, (kinds, LANES)).astype(BF16)
    earlier = iota((kinds, kinds), 1) < iota((kinds, kinds), 0)
    same = iota((kinds, kinds), 1) // half == iota((kinds, kinds), 0) // half
    starts = dot(onehot(earlier), counts)
    inner = dot(onehot(earlier & same), counts)
    position = jnp.concatenate(position, axis=1)
    place = (position + jnp.sum(ones * starts[:, 0:1], axis=0, keepdims=True)).astype(I32)
    position = (position + jnp.sum(ones * inner[:, 0:1], axis=0, keepdims=True)).astype(I32)

    places = onehot(iota((bucket, slots), 0) == position)
    to_block = iota((vol_count, slots), 0) == order
    values = jnp.where(to_block, (low % group_tiles + 1).astype(F32), 0.0)
    rows = lax.dot_general(
        values.astype(BF16), places, (((1,), (1,)), ((), ())), preferred_element_type=F32
    )
    rows = (rows - 1.0).astype(I32)
    per_block = bucket // LANES
    names = jnp.concatenate(
        [rows[b:b + 1, q * LANES:(q + 1) * LANES] for b in range(vol_count) for q in range(per_block)],
        axis=0,
    )
    ids_ref[0:vol_count * per_block, :] = names
    on_lane = iota((kinds, LANES), 0) == iota((kinds, LANES), 1)
    line = jnp.sum(jnp.where(on_lane, starts, 0.0), axis=0, keepdims=True).astype(I32)
    ids_ref[vol_count * per_block:, :] = jnp.broadcast_to(line, (8, LANES))

    part_ref[...] = jnp.zeros_like(part_ref)
    within = iota((WINDOW, BLOCK), 0)
    for copy in small[2:]:
        copy.wait()
    thermal32[...] = thermal_ref[...].astype(F32)
    kinetic32[...] = kinetic_ref[...].astype(F32)

    def base_of(i):
        return slot_smem[lines * i, 0] // 8 * 8

    def add_window(i, base):
        def pair(ref):
            return jnp.concatenate([ref[pl.ds(lines * i + j, 1), :] for j in range(lines)], axis=1)

        base = pl.multiple_of(base, 8)
        match = within + base == pair(slot_ref)
        weights = jnp.concatenate(
            [jnp.where(match, pair(thermal32), 0.0), jnp.where(match, pair(kinetic32), 0.0)], axis=0
        ).astype(BF16)
        sums = dot(weights, kern_ref[pl.ds(pl.multiple_of(i * BLOCK, BLOCK), BLOCK), :])
        part_ref[pl.ds(base, WINDOW), 0:LANES] += sums[:WINDOW]
        part_ref[pl.ds(base, WINDOW), LANES:2 * LANES] += sums[WINDOW:]

    per = blocks // pieces
    for q in range(pieces):
        fetch(q).wait()

        def first_window(i, unused):
            add_window(i, base_of(i))
            return unused

        lax.fori_loop(q * per, (q + 1) * per, first_window, 0, unroll=4)

    def more_windows(i, unused):
        base = base_of(i)
        extra = (slot_smem[lines * i + lines - 1, LANES - 1] - base) // WINDOW

        def one(w, unused):
            add_window(i, base + w * WINDOW)
            return unused

        return lax.fori_loop(1, extra + 1, one, unused)

    lax.fori_loop(0, blocks, more_windows, 0)

    split_ref[...] = halves(part_ref[0:slots, :])

    cols, sub = LANES // half, bucket // half
    lane = iota((sub, LANES), 1) // cols

    def permute(q, unused):
        moved = dot(onehot(iota((bucket, slots), 0) + q * bucket == place), split_ref[...])
        for c in range(2):
            high, low = c * LANES, (c + 2) * LANES
            value = moved[:, high:high + LANES] + moved[:, low:low + LANES]
            rolled = [value] + [pltpu.roll(value, d * cols, 1) for d in range(1, half)]
            for h in range(half):
                packed = rolled[(half - h) % half][0:sub]
                for u in range(1, half):
                    packed = jnp.where(
                        lane == u, rolled[(u - h) % half][u * sub:(u + 1) * sub], packed
                    )
                out_ref[h, c, q] = packed
        return unused

    lax.fori_loop(0, half, permute, 0)


def exchange(
    dims, out_hbm, ids_hbm, gathered, arrived, ids, starts, rows_ref, acc, partial, swapped, sums,
    crossed, total, send_sem, recv_sem, ids_send, ids_recv, local_sem, start_sem, swap_send,
    swap_recv, mid_send, mid_recv, far_send, far_recv, own_sem, pass_send, pass_recv,
):
    vol_count, pix_count, block_tiles, bucket = dims
    half = vol_count // 2
    near_count = 2 * half
    chips = pix_count // 2
    members = chips
    cols, sub = LANES // half, bucket // half
    group_tiles = block_tiles // half
    share = group_tiles // members
    per_block = bucket // LANES
    vol, pix = lax.axis_index("vol"), lax.axis_index("pix")
    side, place = vol // half, vol % half
    chip, core = pix // 2, pix % 2
    group, channel = chip // 2, chip % 2
    member = group * 2 + core
    across = (vol + half) % vol_count
    mine = place * 2 + channel
    sibling = (vol, pix - core + (1 - core))
    id_rows = vol_count * per_block + 1

    def peer(k):
        return (place + k // 2) % half, (channel + k % 2) % 2

    def sender(k):
        return (place + half - k // 2) % half * 2 + (channel + k % 2) % 2

    def pix_of(other_group, other_channel, other_core):
        return (other_group * 2 + other_channel) * 2 + other_core

    barrier = pltpu.get_barrier_semaphore()

    def signal(other_vol, other_pix):
        pl.semaphore_signal(
            barrier, inc=1, device_id=(other_vol, other_pix), device_id_type=MESH
        )

    def greet(k, unused):
        signal(side * half + (place + k // chips) % half, (chip + k % chips) % chips * 2 + core)
        return unused

    signal(across, pix)
    for k in range(1, pix_count):
        signal(vol, (pix + k) % pix_count)
    lax.fori_loop(chips, half * chips, greet, 0)
    pl.semaphore_wait(barrier, pix_count + (half - 1) * chips)

    def target(k):
        other_place, other_channel = peer(k)
        return side * half + other_place, pix_of(group, other_channel, core)

    def rows_copy(q, k):
        other_place, other_channel = peer(k)
        return pltpu.make_async_remote_copy(
            src_ref=out_hbm.at[other_place, other_channel, q], dst_ref=arrived.at[q, mine],
            send_sem=send_sem.at[q, k], recv_sem=recv_sem.at[q, k],
            device_id=target(k), device_id_type=MESH,
        )

    def ids_copy(k):
        return pltpu.make_async_remote_copy(
            src_ref=ids_hbm.at[pl.ds(0, id_rows)], dst_ref=ids.at[mine, pl.ds(0, id_rows)],
            send_sem=ids_send.at[k], recv_sem=ids_recv.at[k],
            device_id=target(k), device_id_type=MESH,
        )

    def local_rows(q):
        return pltpu.make_async_copy(
            out_hbm.at[place, channel, q], arrived.at[q, mine], local_sem.at[q]
        )

    local_ids = pltpu.make_async_copy(ids_hbm, ids.at[mine], local_sem.at[half])

    def send_ids(k, unused):
        ids_copy(k).start()
        return unused

    lax.fori_loop(1, near_count, send_ids, 0)
    local_ids.start()

    def send_chunk(q, unused):
        def one(k, unused):
            rows_copy(q, k).start()
            return unused

        lax.fori_loop(1, near_count, one, 0)
        local_rows(q).start()
        return unused

    lax.fori_loop(0, half, send_chunk, 0)

    def clear(s, unused):
        rows_ref[s, half * bucket:(half + 1) * bucket, :] = jnp.zeros((bucket, LANES), F32)
        return unused

    lax.fori_loop(0, near_count, clear, 0)

    def start_copy(s):
        return pltpu.make_async_copy(
            ids.at[s, pl.ds(vol_count * per_block, 1)], starts.at[pl.ds(s, 1)], start_sem.at[s]
        )

    local_ids.wait()
    start_copy(mine).start()

    def take_ids(k, unused):
        ids_copy(k).wait_recv()
        start_copy(sender(k)).start()
        return unused

    lax.fori_loop(1, near_count, take_ids, 0)

    def take_starts(s, unused):
        start_copy(s).wait()
        return unused

    lax.fori_loop(0, near_count, take_starts, 0)

    lane = iota((1, LANES), 1) // cols
    wide = iota((sub, LANES), 1) // cols
    row = iota((bucket, LANES), 0)
    tile = iota((group_tiles, bucket), 0)

    def unpack(q, s):
        value = arrived[q, s]
        rolled = [value] + [pltpu.roll(value, d * cols, 1) for d in range(1, half)]
        for u in range(half):
            spread = rolled[(half - u) % half]
            for v in range(1, half):
                spread = jnp.where(wide == v, rolled[(v - u) % half], spread)
            first = pl.multiple_of(q * bucket + u * sub, sub)
            rows_ref[s, pl.ds(first, sub), :] = spread

    def accumulate(b, senders):
        places, values = [], []
        for s in senders:
            first = starts[s, b * half]
            low, high = jnp.zeros((1, LANES), I32), jnp.full((1, LANES), bucket, I32)
            for u in range(1, half):
                bound = starts[s, b * half + u] - first
                low = jnp.where(lane == u, bound, low)
                high = jnp.where(lane == u - 1, bound, high)
            keep = (row >= low) & (row < high)
            values.append(halves(jnp.where(keep, rows_ref[s, pl.ds(first, bucket), :], 0.0)))
            names = jnp.concatenate(
                [ids[s, pl.ds(b * per_block + j, 1), :] for j in range(per_block)], axis=1
            )
            places.append(onehot(tile == names))
        acc[...] += dot(jnp.concatenate(places, axis=1), jnp.concatenate(values, axis=0))

    def swap_copy(b, k):
        other = (member + k) % members
        return pltpu.make_async_remote_copy(
            src_ref=partial.at[b, pl.ds(other * share, share)], dst_ref=swapped.at[b, k - 1],
            send_sem=swap_send.at[b, k], recv_sem=swap_recv.at[b, k],
            device_id=(vol, pix_of(other // 2, channel, other % 2)), device_id_type=MESH,
        )

    def swap(b):
        partial[b] = acc[:, :LANES] + acc[:, LANES:]
        for k in range(1, members):
            swap_copy(b, k).start()

    def reduced(b):
        for k in range(1, members):
            swap_copy(b, k).wait_recv()
        value = partial[b, pl.ds(pl.multiple_of(member * share, share), share), :]
        for k in range(1, members):
            value = value + swapped[b, k - 1]
        return value

    def mid_copy(b):
        return pltpu.make_async_remote_copy(
            src_ref=sums.at[b], dst_ref=crossed.at[b],
            send_sem=mid_send.at[b], recv_sem=mid_recv.at[b],
            device_id=(across, pix), device_id_type=MESH,
        )

    def far(q, unused):
        acc[...] = jnp.zeros(acc.shape, F32)

        def one(p, unused):
            @pl.when(p == 0)
            def _():
                local_rows(q).wait()

            @pl.when(p > 0)
            def _():
                rows_copy(q, 2 * p).wait_recv()

            rows_copy(q, 2 * p + 1).wait_recv()
            senders = [sender(2 * p), sender(2 * p + 1)]
            for s in senders:
                unpack(q, s)
            accumulate(q, senders)
            return unused

        lax.fori_loop(0, half, one, 0)
        swap(q)
        sums[q] = reduced(q)
        mid_copy(q).start()
        return unused

    lax.fori_loop(0, half, far, 0)

    def off(i):
        return (i + half - place) % half

    def far_copy(i, k):
        return pltpu.make_async_remote_copy(
            src_ref=total.at[i], dst_ref=gathered.at[core, place, chip],
            send_sem=far_send.at[off(i), k], recv_sem=far_recv.at[off(i), k],
            device_id=(side * half + i, (chip + k) % chips * 2 + core), device_id_type=MESH,
        )

    def own_copy():
        return pltpu.make_async_copy(total.at[place], gathered.at[core, place, chip], own_sem)

    def finalize(i):
        value = reduced(half + i)
        mid_copy(i).wait_recv()
        total[i] = value + crossed[i]

        @pl.when(i != place)
        def _():
            far_copy(i, 0).start()

        @pl.when(i == place)
        def _():
            own_copy().start()

        for k in range(1, chips):
            far_copy(i, k).start()

    def near(i, unused):
        acc[...] = jnp.zeros(acc.shape, F32)

        def some(p, unused):
            accumulate(half + i, [4 * p + j for j in range(4)])
            return unused

        lax.fori_loop(0, near_count // 4, some, 0)
        swap(half + i)

        @pl.when(i > 0)
        def _():
            finalize(i - 1)

        return unused

    lax.fori_loop(0, half, near, 0)
    finalize(half - 1)

    def pass_copy(o, k):
        piece = gathered.at[core, (place + half - o) % half, (chip + chips - k) % chips]
        return pltpu.make_async_remote_copy(
            src_ref=piece, dst_ref=piece,
            send_sem=pass_send.at[o, k], recv_sem=pass_recv.at[o, k],
            device_id=sibling, device_id_type=MESH,
        )

    def far_arrival(o, k):
        return pltpu.make_async_remote_copy(
            src_ref=total.at[0], dst_ref=gathered.at[core, place, chip],
            send_sem=far_send.at[o, k], recv_sem=far_recv.at[o, k],
            device_id=(side * half + (place + o) % half, (chip + k) % chips * 2 + core),
            device_id_type=MESH,
        )

    own_copy().wait()
    pass_copy(0, 0).start()
    for k in range(1, chips):
        far_arrival(0, k).wait_recv()
        pass_copy(0, k).start()

    def relay(o, unused):
        for k in range(chips):
            far_arrival(o, k).wait_recv()
            pass_copy(o, k).start()
        return unused

    lax.fori_loop(1, half, relay, 0)

    def passed(o, unused):
        for k in range(chips):
            pass_copy(o, k).wait()
        return unused

    lax.fori_loop(0, half, passed, 0)
    for k in range(1, chips):
        far_arrival(0, k).wait_send()

    def sent(o, unused):
        for k in range(chips):
            far_arrival(o, k).wait_send()
        return unused

    lax.fori_loop(1, half, sent, 0)

    def sent_rows(k, unused):
        ids_copy(k).wait_send()

        def one(q, unused):
            rows_copy(q, k).wait_send()
            return unused

        lax.fori_loop(0, half, one, 0)
        return unused

    lax.fori_loop(1, near_count, sent_rows, 0)

    def sent_sums(b, unused):
        mid_copy(b).wait_send()
        for k in range(1, members):
            swap_copy(b, k).wait_send()
            swap_copy(half + b, k).wait_send()
        return unused

    lax.fori_loop(0, half, sent_sums, 0)


def finish(
    gathered, rank_ref, owned_hbm, shell_hbm, split_ref, shell_ref, owned_ref, shell_sem, owned_sem,
):
    half, chips, share = gathered.shape[1], gathered.shape[2], gathered.shape[3]
    cols = LANES // half
    owned_most = owned_ref.shape[0]
    block_tiles = shell_ref.shape[0]
    group_tiles = block_tiles // half
    lane = iota((share, LANES), 1) // cols
    for core in range(2):
        for chip in range(chips):
            first, channel = (chip // 2 * 2 + core) * share, chip % 2
            rolled = []
            for s in range(half):
                value = gathered[core, s, chip]
                rolled.append([value] + [pltpu.roll(value, d * cols, 1) for d in range(1, half)])
            for u in range(half):
                value = rolled[0][(half - u) % half]
                for s in range(1, half):
                    value = jnp.where(lane == s, rolled[s][(s - u) % half], value)
                start = u * group_tiles + first
                shell_ref[start:start + share, channel * LANES:(channel + 1) * LANES] = value
                both = halves(value)
                for part in range(2):
                    at = (2 * part + channel) * LANES
                    split_ref[start:start + share, at:at + LANES] = both[:, part * LANES:(part + 1) * LANES]
    shell_copy = pltpu.make_async_copy(shell_ref, shell_hbm, shell_sem)
    shell_copy.start()
    rank = jnp.concatenate([rank_ref[q:q + 1, :] for q in range(rank_ref.shape[0])], axis=1)
    moved = dot(onehot(iota((owned_most, block_tiles), 0) == rank), split_ref[...])
    owned_ref[...] = moved[:, :2 * LANES] + moved[:, 2 * LANES:]
    owned_copy = pltpu.make_async_copy(owned_ref, owned_hbm, owned_sem)
    owned_copy.start()
    shell_copy.wait()
    owned_copy.wait()


def shards(kernel, pressure, velocity, entry_slot, slot_tile, tile_owner):
    vol_count, pix_count = lax.axis_size("vol"), lax.axis_size("pix")
    device_count = vol_count * pix_count
    entries = kernel.shape[0]
    slots = slot_tile.shape[1]
    tiles = tile_owner.shape[0]
    block_tiles = tiles // vol_count
    owned_most = 2 * block_tiles // pix_count
    bucket = 2 * slots // vol_count
    width = 2 * kernel.shape[1]
    vmem = pl.BlockSpec(memory_space=pltpu.VMEM)
    anywhere = pl.BlockSpec(memory_space=pl.ANY)
    hbm = pl.BlockSpec(memory_space=pltpu.HBM)
    dma = pltpu.SemaphoreType.DMA

    shape = (entries // LANES, LANES)
    half = vol_count // 2
    sub = bucket // half
    id_rows = vol_count * bucket // LANES + 8
    outgoing, ids, rank = pl.pallas_call(
        functools.partial(prepare, (vol_count, pix_count, slots, block_tiles, bucket)),
        out_shape=(
            jax.ShapeDtypeStruct((half, 2, half, sub, LANES), F32),
            jax.ShapeDtypeStruct((id_rows, LANES), I32),
            jax.ShapeDtypeStruct((block_tiles // LANES, LANES), I32),
        ),
        in_specs=[hbm] * 6,
        out_specs=(vmem, vmem, vmem),
        scratch_shapes=[
            pltpu.VMEM(kernel.shape, BF16),
            pltpu.SMEM(shape, I32),
            pltpu.VMEM(shape, BF16),
            pltpu.VMEM(shape, BF16),
            pltpu.VMEM(shape, I32),
            pltpu.VMEM((1, slots), I32),
            pltpu.VMEM((block_tiles // LANES, LANES), I32),
            pltpu.VMEM(shape, F32),
            pltpu.VMEM(shape, F32),
            pltpu.VMEM((slots + WINDOW, width), F32),
            pltpu.VMEM((slots, 2 * width), BF16),
            dma((4,)),
            dma((6,)),
        ],
        compiler_params=pltpu.CompilerParams(vmem_limit_bytes=PREPARE_VMEM),
        name="prepare",
    )(*[
        pltpu.with_memory_space_constraint(x, pltpu.HBM) for x in (
            kernel, pressure.reshape(shape), velocity.reshape(shape), entry_slot.reshape(shape),
            slot_tile, tile_owner.reshape(tiles // LANES, LANES),
        )
    ])

    chips = pix_count // 2
    near = vol_count
    group_tiles = block_tiles // half
    share = group_tiles // chips
    gathered = pl.pallas_call(
        functools.partial(exchange, (vol_count, pix_count, block_tiles, bucket)),
        out_shape=jax.ShapeDtypeStruct((2, half, chips, share, LANES), F32),
        in_specs=[anywhere, anywhere],
        out_specs=vmem,
        scratch_shapes=[
            pltpu.VMEM((half, near, sub, LANES), F32),
            pltpu.VMEM((near, id_rows, LANES), I32),
            pltpu.SMEM((near, LANES), I32),
            pltpu.VMEM((near, (half + 1) * bucket, LANES), F32),
            pltpu.VMEM((group_tiles, 2 * LANES), F32),
            pltpu.VMEM((vol_count, group_tiles, LANES), F32),
            pltpu.VMEM((vol_count, chips - 1, share, LANES), F32),
            pltpu.VMEM((half, share, LANES), F32),
            pltpu.VMEM((half, share, LANES), F32),
            pltpu.VMEM((half, share, LANES), F32),
            dma((half, near)), dma((half, near)), dma((near,)), dma((near,)),
            dma((half + 1,)), dma((near,)), dma((vol_count, chips)), dma((vol_count, chips)),
            dma((half,)), dma((half,)), dma((half, chips)), dma((half, chips)), dma,
            dma((half, chips)), dma((half, chips)),
        ],
        compiler_params=pltpu.CompilerParams(
            collective_id=0, has_side_effects=True, vmem_limit_bytes=EXCHANGE_VMEM
        ),
        name="exchange",
    )(outgoing, ids)

    return pl.pallas_call(
        finish,
        out_shape=(
            jax.ShapeDtypeStruct((owned_most, width), F32),
            jax.ShapeDtypeStruct((block_tiles, width), F32),
        ),
        in_specs=[vmem, vmem],
        out_specs=(anywhere, anywhere),
        scratch_shapes=[
            pltpu.VMEM((block_tiles, 2 * width), BF16),
            pltpu.VMEM((block_tiles, width), F32),
            pltpu.VMEM((owned_most, width), F32),
            dma,
            dma,
        ],
        compiler_params=pltpu.CompilerParams(vmem_limit_bytes=FINISH_VMEM),
        name="finish",
    )(gathered, rank)


def solution(mesh):
    in_specs = (
        P(("vol", "pix"), None),
        P(("vol", "pix")),
        P(("vol", "pix")),
        P(("vol", "pix"), None),
        P(("vol", "pix"), None),
        P(),
    )
    out_specs = (P(("vol", "pix"), None), P("vol", None))
    return jax.shard_map(shards, mesh=mesh, in_specs=in_specs, out_specs=out_specs, check_vma=False)
```

```python
import functools

import jax
import jax.numpy as jnp
from jax import lax
from jax.experimental import pallas as pl
from jax.experimental.pallas import tpu as pltpu
from jax.sharding import PartitionSpec as P

MESH = pl.DeviceIdType.MESH
LANES = 128
BLOCK = 256
WINDOW = 48
F32 = jnp.float32
BF16 = jnp.bfloat16
I32 = jnp.int32
PREPARE_VMEM = 24 << 20
EXCHANGE_VMEM = 24 << 20
FINISH_VMEM = 16 << 20


def iota(shape, axis):
    return lax.broadcasted_iota(I32, shape, axis)


def onehot(mask):
    return jnp.where(mask, 1.0, 0.0).astype(BF16)


def dot(a, b):
    return jnp.dot(a, b, preferred_element_type=F32)


def halves(x):
    high = x.astype(BF16)
    low = (x - high.astype(F32)).astype(BF16)
    return jnp.concatenate([high, low], axis=1)


def prepare(
    dims, kern_hbm, thermal_hbm, kinetic_hbm, slot_hbm, tile_hbm, owner_hbm,
    split_ref, place_ref, ids_ref, rank_ref, kern_ref, slot_smem, thermal_ref, kinetic_ref, slot_ref,
    tile_ref, owner_ref, thermal32, kinetic32, part_ref, sems, small_sem,
):
    vol_count, pix_count, slots, block_tiles, bucket = dims
    entries = kern_ref.shape[0]
    blocks = entries // BLOCK
    pieces = sems.shape[0]
    piece = entries // pieces
    lines = BLOCK // LANES

    block_high = block_tiles // LANES
    first_high = pl.multiple_of(lax.axis_index("vol") * block_high, block_high)
    small = [
        pltpu.make_async_copy(tile_hbm, tile_ref, small_sem.at[0]),
        pltpu.make_async_copy(owner_hbm.at[pl.ds(first_high, block_high)], owner_ref, small_sem.at[1]),
        pltpu.make_async_copy(slot_hbm, slot_smem, small_sem.at[2]),
        pltpu.make_async_copy(slot_hbm, slot_ref, small_sem.at[3]),
        pltpu.make_async_copy(thermal_hbm, thermal_ref, small_sem.at[4]),
        pltpu.make_async_copy(kinetic_hbm, kinetic_ref, small_sem.at[5]),
    ]
    for copy in small:
        copy.start()

    def fetch(q):
        rows = pl.ds(q * piece, piece)
        return pltpu.make_async_copy(kern_hbm.at[rows], kern_ref.at[rows], sems.at[q])

    for q in range(pieces):
        fetch(q).start()

    small[0].wait()
    small[1].wait()
    mine = owner_ref[...] == lax.axis_index("pix")
    ones = jnp.where(mine, 1.0, 0.0)
    upper = onehot(iota((LANES, LANES), 0) < iota((LANES, LANES), 1))
    above = onehot(iota((block_high, block_high), 1) < iota((block_high, block_high), 0))
    total = jnp.broadcast_to(jnp.sum(ones, axis=1, keepdims=True), (block_high, LANES))
    rank = dot(ones.astype(BF16), upper) + dot(above, total.astype(BF16))
    rank_ref[...] = jnp.where(mine, rank, -1.0).astype(I32)

    half = vol_count // 2
    side = lax.axis_index("vol") // half
    tile = tile_ref[...]
    block, low = tile // block_tiles, tile % block_tiles
    order = (block + vol_count - (1 - side) * half) % vol_count
    group_tiles = block_tiles // half
    kinds = vol_count * half
    to_kind = iota((kinds, slots), 0) == order * half + low // group_tiles
    ones = jnp.where(to_kind, 1.0, 0.0)
    carry = jnp.zeros((kinds, 1), F32)
    position = []
    for j in range(slots // LANES):
        chunk = ones[:, j * LANES:(j + 1) * LANES]
        ranks = dot(chunk.astype(BF16), upper) + carry
        position.append(jnp.sum(chunk * ranks, axis=0, keepdims=True))
        carry = carry + jnp.sum(chunk, axis=1, keepdims=True)
    counts = jnp.broadcast_to(carry, (kinds, LANES)).astype(BF16)
    earlier = iota((kinds, kinds), 1) < iota((kinds, kinds), 0)
    same = iota((kinds, kinds), 1) // half == iota((kinds, kinds), 0) // half
    starts = dot(onehot(earlier), counts)
    inner = dot(onehot(earlier & same), counts)
    position = jnp.concatenate(position, axis=1)
    place_ref[...] = (position + jnp.sum(ones * starts[:, 0:1], axis=0, keepdims=True)).astype(I32)
    position = (position + jnp.sum(ones * inner[:, 0:1], axis=0, keepdims=True)).astype(I32)

    places = onehot(iota((bucket, slots), 0) == position)
    to_block = iota((vol_count, slots), 0) == order
    values = jnp.where(to_block, (low % group_tiles + 1).astype(F32), 0.0)
    rows = lax.dot_general(
        values.astype(BF16), places, (((1,), (1,)), ((), ())), preferred_element_type=F32
    )
    rows = (rows - 1.0).astype(I32)
    per_block = bucket // LANES
    names = jnp.concatenate(
        [rows[b:b + 1, q * LANES:(q + 1) * LANES] for b in range(vol_count) for q in range(per_block)],
        axis=0,
    )
    ids_ref[0:vol_count * per_block, :] = names
    on_lane = iota((kinds, LANES), 0) == iota((kinds, LANES), 1)
    line = jnp.sum(jnp.where(on_lane, starts, 0.0), axis=0, keepdims=True).astype(I32)
    ids_ref[vol_count * per_block:, :] = jnp.broadcast_to(line, (8, LANES))

    part_ref[...] = jnp.zeros_like(part_ref)
    within = iota((WINDOW, BLOCK), 0)
    for copy in small[2:]:
        copy.wait()
    thermal32[...] = thermal_ref[...].astype(F32)
    kinetic32[...] = kinetic_ref[...].astype(F32)

    def base_of(i):
        return slot_smem[lines * i, 0] // 8 * 8

    def add_window(i, base):
        def pair(ref):
            return jnp.concatenate([ref[pl.ds(lines * i + j, 1), :] for j in range(lines)], axis=1)

        base = pl.multiple_of(base, 8)
        match = within + base == pair(slot_ref)
        weights = jnp.concatenate(
            [jnp.where(match, pair(thermal32), 0.0), jnp.where(match, pair(kinetic32), 0.0)], axis=0
        ).astype(BF16)
        sums = dot(weights, kern_ref[pl.ds(pl.multiple_of(i * BLOCK, BLOCK), BLOCK), :])
        part_ref[pl.ds(base, WINDOW), 0:LANES] += sums[:WINDOW]
        part_ref[pl.ds(base, WINDOW), LANES:2 * LANES] += sums[WINDOW:]

    per = blocks // pieces
    for q in range(pieces):
        fetch(q).wait()

        def first_window(i, unused):
            add_window(i, base_of(i))
            return unused

        lax.fori_loop(q * per, (q + 1) * per, first_window, 0, unroll=16)

    def more_windows(i, unused):
        base = base_of(i)
        extra = (slot_smem[lines * i + lines - 1, LANES - 1] - base) // WINDOW

        def one(w, unused):
            add_window(i, base + w * WINDOW)
            return unused

        return lax.fori_loop(1, extra + 1, one, unused)

    rows = slot_ref.shape[0] - lines + 1
    ends = pltpu.roll(slot_ref[lines - 1:, :], 1, 1)
    spans = ends - slot_ref[0:rows, :] // 8 * 8
    first = (iota((rows, LANES), 1) == 0) & (iota((rows, LANES), 0) % lines == 0)

    @pl.when(jnp.max(jnp.where(first, spans, 0)) >= WINDOW)
    def _():
        lax.fori_loop(0, blocks, more_windows, 0)

    split_ref[...] = halves(part_ref[0:slots, :])


def exchange(
    dims, split_ref, place_ref, ids_hbm, gathered, out_ref, arrived, ids, starts, rows_ref, acc, partial, swapped, sums,
    crossed, total, send_sem, recv_sem, ids_send, ids_recv, local_sem, start_sem, swap_send,
    swap_recv, mid_send, mid_recv, far_send, far_recv, own_sem, pass_send, pass_recv,
):
    vol_count, pix_count, block_tiles, bucket = dims
    half = vol_count // 2
    near_count = 2 * half
    chips = pix_count // 2
    members = chips
    cols, sub = LANES // half, bucket // half
    group_tiles = block_tiles // half
    share = group_tiles // members
    per_block = bucket // LANES
    vol, pix = lax.axis_index("vol"), lax.axis_index("pix")
    side, place = vol // half, vol % half
    chip, core = pix // 2, pix % 2
    group, channel = chip // 2, chip % 2
    member = group * 2 + core
    across = (vol + half) % vol_count
    mine = place * 2 + channel
    sibling = (vol, pix - core + (1 - core))
    id_rows = vol_count * per_block + 1

    def peer(k):
        return (place + k // 2) % half, (channel + k % 2) % 2

    def sender(k):
        return (place + half - k // 2) % half * 2 + (channel + k % 2) % 2

    def pix_of(other_group, other_channel, other_core):
        return (other_group * 2 + other_channel) * 2 + other_core

    barrier = pltpu.get_barrier_semaphore()

    def signal(other_vol, other_pix):
        pl.semaphore_signal(
            barrier, inc=1, device_id=(other_vol, other_pix), device_id_type=MESH
        )

    def greet(k, unused):
        signal(side * half + (place + k // chips) % half, (chip + k % chips) % chips * 2 + core)
        return unused

    signal(across, pix)
    for k in range(1, pix_count):
        signal(vol, (pix + k) % pix_count)
    lax.fori_loop(chips, half * chips, greet, 0)

    wide = iota((sub, LANES), 1) // cols
    slots = place_ref.shape[1]

    def permute(q):
        moved = dot(onehot(iota((bucket, slots), 0) + q * bucket == place_ref[...]), split_ref[...])
        for c in range(2):
            high, low = c * LANES, (c + 2) * LANES
            value = moved[:, high:high + LANES] + moved[:, low:low + LANES]
            rolled = [value] + [pltpu.roll(value, d * cols, 1) for d in range(1, half)]
            for h in range(half):
                packed = rolled[(half - h) % half][0:sub]
                for u in range(1, half):
                    packed = jnp.where(
                        wide == u, rolled[(u - h) % half][u * sub:(u + 1) * sub], packed
                    )
                out_ref[h, c, q] = packed

    permute(0)
    pl.semaphore_wait(barrier, pix_count + (half - 1) * chips)

    def target(k):
        other_place, other_channel = peer(k)
        return side * half + other_place, pix_of(group, other_channel, core)

    def rows_copy(q, k):
        other_place, other_channel = peer(k)
        return pltpu.make_async_remote_copy(
            src_ref=out_ref.at[other_place, other_channel, q], dst_ref=arrived.at[q, mine],
            send_sem=send_sem.at[q, k], recv_sem=recv_sem.at[q, k],
            device_id=target(k), device_id_type=MESH,
        )

    def ids_copy(k):
        return pltpu.make_async_remote_copy(
            src_ref=ids_hbm.at[pl.ds(0, id_rows)], dst_ref=ids.at[mine, pl.ds(0, id_rows)],
            send_sem=ids_send.at[k], recv_sem=ids_recv.at[k],
            device_id=target(k), device_id_type=MESH,
        )

    def local_rows(q):
        return pltpu.make_async_copy(
            out_ref.at[place, channel, q], arrived.at[q, mine], local_sem.at[q]
        )

    local_ids = pltpu.make_async_copy(ids_hbm, ids.at[mine], local_sem.at[half])

    def send_ids(k, unused):
        ids_copy(k).start()
        return unused

    lax.fori_loop(1, near_count, send_ids, 0)
    local_ids.start()

    def send_chunk(q, unused):
        @pl.when(q > 0)
        def _():
            permute(q)

        def one(k, unused):
            rows_copy(q, k).start()
            return unused

        lax.fori_loop(1, near_count, one, 0)
        local_rows(q).start()
        return unused

    lax.fori_loop(0, half, send_chunk, 0)

    def clear(s, unused):
        rows_ref[s, half * bucket:(half + 1) * bucket, :] = jnp.zeros((bucket, LANES), F32)
        return unused

    lax.fori_loop(0, near_count, clear, 0)

    def start_copy(s):
        return pltpu.make_async_copy(
            ids.at[s, pl.ds(vol_count * per_block, 1)], starts.at[pl.ds(s, 1)], start_sem.at[s]
        )

    local_ids.wait()
    start_copy(mine).start()

    def take_ids(k, unused):
        ids_copy(k).wait_recv()
        start_copy(sender(k)).start()
        return unused

    lax.fori_loop(1, near_count, take_ids, 0)

    def take_starts(s, unused):
        start_copy(s).wait()
        return unused

    lax.fori_loop(0, near_count, take_starts, 0)

    lane = iota((1, LANES), 1) // cols
    row = iota((bucket, LANES), 0)
    tile = iota((group_tiles, bucket), 0)

    def unpack(q, s):
        value = arrived[q, s]
        rolled = [value] + [pltpu.roll(value, d * cols, 1) for d in range(1, half)]
        for u in range(half):
            spread = rolled[(half - u) % half]
            for v in range(1, half):
                spread = jnp.where(wide == v, rolled[(v - u) % half], spread)
            first = pl.multiple_of(q * bucket + u * sub, sub)
            rows_ref[s, pl.ds(first, sub), :] = spread

    def accumulate(b, senders):
        places, values = [], []
        for s in senders:
            first = starts[s, b * half]
            low, high = jnp.zeros((1, LANES), I32), jnp.full((1, LANES), bucket, I32)
            for u in range(1, half):
                bound = starts[s, b * half + u] - first
                low = jnp.where(lane == u, bound, low)
                high = jnp.where(lane == u - 1, bound, high)
            keep = (row >= low) & (row < high)
            values.append(halves(jnp.where(keep, rows_ref[s, pl.ds(first, bucket), :], 0.0)))
            names = jnp.concatenate(
                [ids[s, pl.ds(b * per_block + j, 1), :] for j in range(per_block)], axis=1
            )
            places.append(onehot(tile == names))
        acc[...] += dot(jnp.concatenate(places, axis=1), jnp.concatenate(values, axis=0))

    def swap_copy(b, k):
        other = (member + k) % members
        return pltpu.make_async_remote_copy(
            src_ref=partial.at[b, pl.ds(other * share, share)], dst_ref=swapped.at[b, k - 1],
            send_sem=swap_send.at[b, k], recv_sem=swap_recv.at[b, k],
            device_id=(vol, pix_of(other // 2, channel, other % 2)), device_id_type=MESH,
        )

    def swap(b):
        partial[b] = acc[:, :LANES] + acc[:, LANES:]
        for k in range(1, members):
            swap_copy(b, k).start()

    def reduced(b):
        for k in range(1, members):
            swap_copy(b, k).wait_recv()
        value = partial[b, pl.ds(pl.multiple_of(member * share, share), share), :]
        for k in range(1, members):
            value = value + swapped[b, k - 1]
        return value

    def mid_copy(b):
        return pltpu.make_async_remote_copy(
            src_ref=sums.at[b], dst_ref=crossed.at[b],
            send_sem=mid_send.at[b], recv_sem=mid_recv.at[b],
            device_id=(across, pix), device_id_type=MESH,
        )

    def far(q, unused):
        acc[...] = jnp.zeros(acc.shape, F32)

        def one(p, unused):
            @pl.when(p == 0)
            def _():
                local_rows(q).wait()

            @pl.when(p > 0)
            def _():
                rows_copy(q, 2 * p).wait_recv()

            rows_copy(q, 2 * p + 1).wait_recv()
            senders = [sender(2 * p), sender(2 * p + 1)]
            for s in senders:
                unpack(q, s)
            accumulate(q, senders)
            return unused

        lax.fori_loop(0, half, one, 0)
        swap(q)
        sums[q] = reduced(q)
        mid_copy(q).start()
        return unused

    lax.fori_loop(0, half, far, 0)

    def off(i):
        return (i + half - place) % half

    def far_copy(i, k):
        return pltpu.make_async_remote_copy(
            src_ref=total.at[i], dst_ref=gathered.at[core, place, chip],
            send_sem=far_send.at[off(i), k], recv_sem=far_recv.at[off(i), k],
            device_id=(side * half + i, (chip + k) % chips * 2 + core), device_id_type=MESH,
        )

    def own_copy():
        return pltpu.make_async_copy(total.at[place], gathered.at[core, place, chip], own_sem)

    def finalize(i):
        value = reduced(half + i)
        mid_copy(i).wait_recv()
        total[i] = value + crossed[i]

        @pl.when(i != place)
        def _():
            far_copy(i, 0).start()

        @pl.when(i == place)
        def _():
            own_copy().start()

        for k in range(1, chips):
            far_copy(i, k).start()

    def near(i, unused):
        acc[...] = jnp.zeros(acc.shape, F32)

        def some(p, unused):
            accumulate(half + i, [4 * p + j for j in range(4)])
            return unused

        lax.fori_loop(0, near_count // 4, some, 0)
        swap(half + i)

        @pl.when(i > 0)
        def _():
            finalize(i - 1)

        return unused

    lax.fori_loop(0, half, near, 0)
    finalize(half - 1)

    def pass_copy(o, k):
        piece = gathered.at[core, (place + half - o) % half, (chip + chips - k) % chips]
        return pltpu.make_async_remote_copy(
            src_ref=piece, dst_ref=piece,
            send_sem=pass_send.at[o, k], recv_sem=pass_recv.at[o, k],
            device_id=sibling, device_id_type=MESH,
        )

    def far_arrival(o, k):
        return pltpu.make_async_remote_copy(
            src_ref=total.at[0], dst_ref=gathered.at[core, place, chip],
            send_sem=far_send.at[o, k], recv_sem=far_recv.at[o, k],
            device_id=(side * half + (place + o) % half, (chip + k) % chips * 2 + core),
            device_id_type=MESH,
        )

    own_copy().wait()
    pass_copy(0, 0).start()
    for k in range(1, chips):
        far_arrival(0, k).wait_recv()
        pass_copy(0, k).start()

    def relay(o, unused):
        for k in range(chips):
            far_arrival(o, k).wait_recv()
            pass_copy(o, k).start()
        return unused

    lax.fori_loop(1, half, relay, 0)

    def passed(o, unused):
        for k in range(chips):
            pass_copy(o, k).wait()
        return unused

    lax.fori_loop(0, half, passed, 0)
    for k in range(1, chips):
        far_arrival(0, k).wait_send()

    def sent(o, unused):
        for k in range(chips):
            far_arrival(o, k).wait_send()
        return unused

    lax.fori_loop(1, half, sent, 0)

    def sent_rows(k, unused):
        ids_copy(k).wait_send()

        def one(q, unused):
            rows_copy(q, k).wait_send()
            return unused

        lax.fori_loop(0, half, one, 0)
        return unused

    lax.fori_loop(1, near_count, sent_rows, 0)

    def sent_sums(b, unused):
        mid_copy(b).wait_send()
        for k in range(1, members):
            swap_copy(b, k).wait_send()
            swap_copy(half + b, k).wait_send()
        return unused

    lax.fori_loop(0, half, sent_sums, 0)


def finish(
    gathered, rank_ref, owned_hbm, shell_hbm, split_ref, shell_ref, owned_ref, shell_sem, owned_sem,
):
    half, chips, share = gathered.shape[1], gathered.shape[2], gathered.shape[3]
    cols = LANES // half
    owned_most = owned_ref.shape[0]
    block_tiles = shell_ref.shape[0]
    group_tiles = block_tiles // half
    lane = iota((share, LANES), 1) // cols
    for core in range(2):
        for chip in range(chips):
            first, channel = (chip // 2 * 2 + core) * share, chip % 2
            rolled = []
            for s in range(half):
                value = gathered[core, s, chip]
                rolled.append([value] + [pltpu.roll(value, d * cols, 1) for d in range(1, half)])
            for u in range(half):
                value = rolled[0][(half - u) % half]
                for s in range(1, half):
                    value = jnp.where(lane == s, rolled[s][(s - u) % half], value)
                start = u * group_tiles + first
                shell_ref[start:start + share, channel * LANES:(channel + 1) * LANES] = value
                both = halves(value)
                for part in range(2):
                    at = (2 * part + channel) * LANES
                    split_ref[start:start + share, at:at + LANES] = both[:, part * LANES:(part + 1) * LANES]
    shell_copy = pltpu.make_async_copy(shell_ref, shell_hbm, shell_sem)
    shell_copy.start()
    rank = jnp.concatenate([rank_ref[q:q + 1, :] for q in range(rank_ref.shape[0])], axis=1)
    moved = dot(onehot(iota((owned_most, block_tiles), 0) == rank), split_ref[...])
    owned_ref[...] = moved[:, :2 * LANES] + moved[:, 2 * LANES:]
    owned_copy = pltpu.make_async_copy(owned_ref, owned_hbm, owned_sem)
    owned_copy.start()
    shell_copy.wait()
    owned_copy.wait()


def shards(kernel, pressure, velocity, entry_slot, slot_tile, tile_owner):
    vol_count, pix_count = lax.axis_size("vol"), lax.axis_size("pix")
    device_count = vol_count * pix_count
    entries = kernel.shape[0]
    slots = slot_tile.shape[1]
    tiles = tile_owner.shape[0]
    block_tiles = tiles // vol_count
    owned_most = 2 * block_tiles // pix_count
    bucket = 2 * slots // vol_count
    width = 2 * kernel.shape[1]
    vmem = pl.BlockSpec(memory_space=pltpu.VMEM)
    anywhere = pl.BlockSpec(memory_space=pl.ANY)
    hbm = pl.BlockSpec(memory_space=pltpu.HBM)
    dma = pltpu.SemaphoreType.DMA

    shape = (entries // LANES, LANES)
    half = vol_count // 2
    sub = bucket // half
    id_rows = vol_count * bucket // LANES + 8
    split, place, ids, rank = pl.pallas_call(
        functools.partial(prepare, (vol_count, pix_count, slots, block_tiles, bucket)),
        out_shape=(
            jax.ShapeDtypeStruct((slots, 2 * width), BF16),
            jax.ShapeDtypeStruct((1, slots), I32),
            jax.ShapeDtypeStruct((id_rows, LANES), I32),
            jax.ShapeDtypeStruct((block_tiles // LANES, LANES), I32),
        ),
        in_specs=[hbm] * 6,
        out_specs=(vmem, vmem, vmem, vmem),
        scratch_shapes=[
            pltpu.VMEM(kernel.shape, BF16),
            pltpu.SMEM(shape, I32),
            pltpu.VMEM(shape, BF16),
            pltpu.VMEM(shape, BF16),
            pltpu.VMEM(shape, I32),
            pltpu.VMEM((1, slots), I32),
            pltpu.VMEM((block_tiles // LANES, LANES), I32),
            pltpu.VMEM(shape, F32),
            pltpu.VMEM(shape, F32),
            pltpu.VMEM((slots + WINDOW, width), F32),
            dma((4,)),
            dma((6,)),
        ],
        compiler_params=pltpu.CompilerParams(vmem_limit_bytes=PREPARE_VMEM),
        name="prepare",
    )(*[
        pltpu.with_memory_space_constraint(x, pltpu.HBM) for x in (
            kernel, pressure.reshape(shape), velocity.reshape(shape), entry_slot.reshape(shape),
            slot_tile, tile_owner.reshape(tiles // LANES, LANES),
        )
    ])

    chips = pix_count // 2
    near = vol_count
    group_tiles = block_tiles // half
    share = group_tiles // chips
    gathered = pl.pallas_call(
        functools.partial(exchange, (vol_count, pix_count, block_tiles, bucket)),
        out_shape=jax.ShapeDtypeStruct((2, half, chips, share, LANES), F32),
        in_specs=[vmem, vmem, anywhere],
        out_specs=vmem,
        scratch_shapes=[
            pltpu.VMEM((half, 2, half, sub, LANES), F32),
            pltpu.VMEM((half, near, sub, LANES), F32),
            pltpu.VMEM((near, id_rows, LANES), I32),
            pltpu.SMEM((near, LANES), I32),
            pltpu.VMEM((near, (half + 1) * bucket, LANES), F32),
            pltpu.VMEM((group_tiles, 2 * LANES), F32),
            pltpu.VMEM((vol_count, group_tiles, LANES), F32),
            pltpu.VMEM((vol_count, chips - 1, share, LANES), F32),
            pltpu.VMEM((half, share, LANES), F32),
            pltpu.VMEM((half, share, LANES), F32),
            pltpu.VMEM((half, share, LANES), F32),
            dma((half, near)), dma((half, near)), dma((near,)), dma((near,)),
            dma((half + 1,)), dma((near,)), dma((vol_count, chips)), dma((vol_count, chips)),
            dma((half,)), dma((half,)), dma((half, chips)), dma((half, chips)), dma,
            dma((half, chips)), dma((half, chips)),
        ],
        compiler_params=pltpu.CompilerParams(
            collective_id=0, has_side_effects=True, vmem_limit_bytes=EXCHANGE_VMEM
        ),
        name="exchange",
    )(split, place, ids)

    return pl.pallas_call(
        finish,
        out_shape=(
            jax.ShapeDtypeStruct((owned_most, width), F32),
            jax.ShapeDtypeStruct((block_tiles, width), F32),
        ),
        in_specs=[vmem, vmem],
        out_specs=(anywhere, anywhere),
        scratch_shapes=[
            pltpu.VMEM((block_tiles, 2 * width), BF16),
            pltpu.VMEM((block_tiles, width), F32),
            pltpu.VMEM((owned_most, width), F32),
            dma,
            dma,
        ],
        compiler_params=pltpu.CompilerParams(vmem_limit_bytes=FINISH_VMEM),
        name="finish",
    )(gathered, rank)


def solution(mesh):
    in_specs = (
        P(("vol", "pix"), None),
        P(("vol", "pix")),
        P(("vol", "pix")),
        P(("vol", "pix"), None),
        P(("vol", "pix"), None),
        P(),
    )
    out_specs = (P(("vol", "pix"), None), P("vol", None))
    return jax.shard_map(shards, mesh=mesh, in_specs=in_specs, out_specs=out_specs, check_vma=False)
```

```python
import functools

import jax
import jax.numpy as jnp
from jax import lax
from jax.experimental import pallas as pl
from jax.experimental.pallas import tpu as pltpu
from jax.sharding import PartitionSpec as P

MESH = pl.DeviceIdType.MESH
LANES = 128
BLOCK = 256
WINDOW = 48
F32 = jnp.float32
BF16 = jnp.bfloat16
I32 = jnp.int32
PREPARE_VMEM = 24 << 20
EXCHANGE_VMEM = 24 << 20
FINISH_VMEM = 16 << 20


def iota(shape, axis):
    return lax.broadcasted_iota(I32, shape, axis)


def onehot(mask):
    return jnp.where(mask, 1.0, 0.0).astype(BF16)


def dot(a, b):
    return jnp.dot(a, b, preferred_element_type=F32)


def halves(x):
    high = x.astype(BF16)
    low = (x - high.astype(F32)).astype(BF16)
    return jnp.concatenate([high, low], axis=1)


def turn_groups(values, lane, cols):
    values = list(values)
    step = 1
    while step < len(values):
        upper = lane // step % 2 == 1
        for i in range(len(values)):
            if i // step % 2 == 0:
                a, b = values[i], values[i + step]
                values[i] = jnp.where(upper, pltpu.roll(b, step * cols, 1), a)
                values[i + step] = jnp.where(upper, b, pltpu.roll(a, LANES - step * cols, 1))
        step *= 2
    return values


def prepare(
    dims, kern_hbm, thermal_hbm, kinetic_hbm, slot_hbm, tile_hbm, owner_hbm,
    split_ref, place_ref, ids_ref, rank_ref, kern_ref, slot_smem, thermal_ref, kinetic_ref, slot_ref,
    tile_ref, owner_ref, thermal32, kinetic32, part_ref, sems, small_sem,
):
    vol_count, pix_count, slots, block_tiles, bucket = dims
    entries = kern_ref.shape[0]
    blocks = entries // BLOCK
    pieces = sems.shape[0]
    piece = entries // pieces
    lines = BLOCK // LANES

    block_high = block_tiles // LANES
    first_high = pl.multiple_of(lax.axis_index("vol") * block_high, block_high)
    small = [
        pltpu.make_async_copy(tile_hbm, tile_ref, small_sem.at[0]),
        pltpu.make_async_copy(owner_hbm.at[pl.ds(first_high, block_high)], owner_ref, small_sem.at[1]),
        pltpu.make_async_copy(slot_hbm, slot_smem, small_sem.at[2]),
        pltpu.make_async_copy(slot_hbm, slot_ref, small_sem.at[3]),
        pltpu.make_async_copy(thermal_hbm, thermal_ref, small_sem.at[4]),
        pltpu.make_async_copy(kinetic_hbm, kinetic_ref, small_sem.at[5]),
    ]
    for copy in small:
        copy.start()

    def fetch(q):
        rows = pl.ds(q * piece, piece)
        return pltpu.make_async_copy(kern_hbm.at[rows], kern_ref.at[rows], sems.at[q])

    for q in range(pieces):
        fetch(q).start()

    small[0].wait()
    small[1].wait()
    mine = owner_ref[...] == lax.axis_index("pix")
    ones = jnp.where(mine, 1.0, 0.0)
    upper = onehot(iota((LANES, LANES), 0) < iota((LANES, LANES), 1))
    above = onehot(iota((block_high, block_high), 1) < iota((block_high, block_high), 0))
    total = jnp.broadcast_to(jnp.sum(ones, axis=1, keepdims=True), (block_high, LANES))
    rank = dot(ones.astype(BF16), upper) + dot(above, total.astype(BF16))
    rank_ref[...] = jnp.where(mine, rank, -1.0).astype(I32)

    half = vol_count // 2
    side = lax.axis_index("vol") // half
    tile = tile_ref[...]
    block, low = tile // block_tiles, tile % block_tiles
    order = (block + vol_count - (1 - side) * half) % vol_count
    group_tiles = block_tiles // half
    kinds = vol_count * half
    to_kind = iota((kinds, slots), 0) == order * half + low // group_tiles
    ones = jnp.where(to_kind, 1.0, 0.0)
    carry = jnp.zeros((kinds, 1), F32)
    position = []
    for j in range(slots // LANES):
        chunk = ones[:, j * LANES:(j + 1) * LANES]
        ranks = dot(chunk.astype(BF16), upper) + carry
        position.append(jnp.sum(chunk * ranks, axis=0, keepdims=True))
        carry = carry + jnp.sum(chunk, axis=1, keepdims=True)
    counts = jnp.broadcast_to(carry, (kinds, LANES)).astype(BF16)
    earlier = iota((kinds, kinds), 1) < iota((kinds, kinds), 0)
    same = iota((kinds, kinds), 1) // half == iota((kinds, kinds), 0) // half
    starts = dot(onehot(earlier), counts)
    inner = dot(onehot(earlier & same), counts)
    position = jnp.concatenate(position, axis=1)
    place_ref[...] = (position + jnp.sum(ones * starts[:, 0:1], axis=0, keepdims=True)).astype(I32)
    position = (position + jnp.sum(ones * inner[:, 0:1], axis=0, keepdims=True)).astype(I32)

    places = onehot(iota((bucket, slots), 0) == position)
    to_block = iota((vol_count, slots), 0) == order
    values = jnp.where(to_block, (low % group_tiles + 1).astype(F32), 0.0)
    rows = lax.dot_general(
        values.astype(BF16), places, (((1,), (1,)), ((), ())), preferred_element_type=F32
    )
    rows = (rows - 1.0).astype(I32)
    per_block = bucket // LANES
    names = jnp.concatenate(
        [rows[b:b + 1, q * LANES:(q + 1) * LANES] for b in range(vol_count) for q in range(per_block)],
        axis=0,
    )
    ids_ref[0:vol_count * per_block, :] = names
    on_lane = iota((kinds, LANES), 0) == iota((kinds, LANES), 1)
    line = jnp.sum(jnp.where(on_lane, starts, 0.0), axis=0, keepdims=True).astype(I32)
    ids_ref[vol_count * per_block:, :] = jnp.broadcast_to(line, (8, LANES))

    part_ref[...] = jnp.zeros_like(part_ref)
    within = iota((WINDOW, BLOCK), 0)
    for copy in small[2:]:
        copy.wait()
    thermal32[...] = thermal_ref[...].astype(F32)
    kinetic32[...] = kinetic_ref[...].astype(F32)

    def base_of(i):
        return slot_smem[lines * i, 0] // 8 * 8

    def add_window(i, base):
        def pair(ref):
            return jnp.concatenate([ref[pl.ds(lines * i + j, 1), :] for j in range(lines)], axis=1)

        base = pl.multiple_of(base, 8)
        match = within + base == pair(slot_ref)
        weights = jnp.concatenate(
            [jnp.where(match, pair(thermal32), 0.0), jnp.where(match, pair(kinetic32), 0.0)], axis=0
        ).astype(BF16)
        sums = dot(weights, kern_ref[pl.ds(pl.multiple_of(i * BLOCK, BLOCK), BLOCK), :])
        part_ref[pl.ds(base, WINDOW), 0:LANES] += sums[:WINDOW]
        part_ref[pl.ds(base, WINDOW), LANES:2 * LANES] += sums[WINDOW:]

    per = blocks // pieces
    for q in range(pieces):
        fetch(q).wait()

        def first_window(i, unused):
            add_window(i, base_of(i))
            return unused

        lax.fori_loop(q * per, (q + 1) * per, first_window, 0, unroll=16)

    def more_windows(i, unused):
        base = base_of(i)
        extra = (slot_smem[lines * i + lines - 1, LANES - 1] - base) // WINDOW

        def one(w, unused):
            add_window(i, base + w * WINDOW)
            return unused

        return lax.fori_loop(1, extra + 1, one, unused)

    rows = slot_ref.shape[0] - lines + 1
    ends = pltpu.roll(slot_ref[lines - 1:, :], 1, 1)
    spans = ends - slot_ref[0:rows, :] // 8 * 8
    first = (iota((rows, LANES), 1) == 0) & (iota((rows, LANES), 0) % lines == 0)

    @pl.when(jnp.max(jnp.where(first, spans, 0)) >= WINDOW)
    def _():
        lax.fori_loop(0, blocks, more_windows, 0)

    split_ref[...] = halves(part_ref[0:slots, :])


def exchange(
    dims, split_ref, place_ref, ids_hbm, gathered, out_ref, arrived, ids, starts, rows_ref, acc, partial, swapped, sums,
    crossed, total, send_sem, recv_sem, ids_send, ids_recv, local_sem, start_sem, swap_send,
    swap_recv, mid_send, mid_recv, far_send, far_recv, own_sem, pass_send, pass_recv,
):
    vol_count, pix_count, block_tiles, bucket = dims
    half = vol_count // 2
    near_count = 2 * half
    chips = pix_count // 2
    members = chips
    cols, sub = LANES // half, bucket // half
    group_tiles = block_tiles // half
    share = group_tiles // members
    per_block = bucket // LANES
    vol, pix = lax.axis_index("vol"), lax.axis_index("pix")
    side, place = vol // half, vol % half
    chip, core = pix // 2, pix % 2
    group, channel = chip // 2, chip % 2
    member = group * 2 + core
    across = (vol + half) % vol_count
    mine = place * 2 + channel
    sibling = (vol, pix - core + (1 - core))
    id_rows = vol_count * per_block + 1

    def peer(k):
        return (place + k // 2) % half, (channel + k % 2) % 2

    def sender(k):
        return (place + half - k // 2) % half * 2 + (channel + k % 2) % 2

    def pix_of(other_group, other_channel, other_core):
        return (other_group * 2 + other_channel) * 2 + other_core

    barrier = pltpu.get_barrier_semaphore()

    def signal(other_vol, other_pix):
        pl.semaphore_signal(
            barrier, inc=1, device_id=(other_vol, other_pix), device_id_type=MESH
        )

    def greet(k, unused):
        signal(side * half + (place + k // chips) % half, (chip + k % chips) % chips * 2 + core)
        return unused

    signal(across, pix)
    for k in range(1, pix_count):
        signal(vol, (pix + k) % pix_count)
    lax.fori_loop(chips, half * chips, greet, 0)

    wide = iota((sub, LANES), 1) // cols
    slots = place_ref.shape[1]

    def permute(q):
        moved = dot(onehot(iota((bucket, slots), 0) + q * bucket == place_ref[...]), split_ref[...])
        for c in range(2):
            high, low = c * LANES, (c + 2) * LANES
            value = moved[:, high:high + LANES] + moved[:, low:low + LANES]
            parts = [value[u * sub:(u + 1) * sub] for u in range(half)]
            for h, packed in enumerate(turn_groups(parts, wide, cols)):
                out_ref[h, c, q] = packed

    permute(0)
    pl.semaphore_wait(barrier, pix_count + (half - 1) * chips)

    def target(k):
        other_place, other_channel = peer(k)
        return side * half + other_place, pix_of(group, other_channel, core)

    def rows_copy(q, k):
        other_place, other_channel = peer(k)
        return pltpu.make_async_remote_copy(
            src_ref=out_ref.at[other_place, other_channel, q], dst_ref=arrived.at[q, mine],
            send_sem=send_sem.at[q, k], recv_sem=recv_sem.at[q, k],
            device_id=target(k), device_id_type=MESH,
        )

    def ids_copy(k):
        return pltpu.make_async_remote_copy(
            src_ref=ids_hbm.at[pl.ds(0, id_rows)], dst_ref=ids.at[mine, pl.ds(0, id_rows)],
            send_sem=ids_send.at[k], recv_sem=ids_recv.at[k],
            device_id=target(k), device_id_type=MESH,
        )

    def local_rows(q):
        return pltpu.make_async_copy(
            out_ref.at[place, channel, q], arrived.at[q, mine], local_sem.at[q]
        )

    local_ids = pltpu.make_async_copy(ids_hbm, ids.at[mine], local_sem.at[half])

    def send_ids(k, unused):
        ids_copy(k).start()
        return unused

    lax.fori_loop(1, near_count, send_ids, 0)
    local_ids.start()

    def send_chunk(q, unused):
        @pl.when(q > 0)
        def _():
            permute(q)

        def one(k, unused):
            rows_copy(q, k).start()
            return unused

        lax.fori_loop(1, near_count, one, 0)
        local_rows(q).start()
        return unused

    lax.fori_loop(0, half, send_chunk, 0)

    def clear(s, unused):
        rows_ref[s, half * bucket:(half + 1) * bucket, :] = jnp.zeros((bucket, LANES), F32)
        return unused

    lax.fori_loop(0, near_count, clear, 0)

    def start_copy(s):
        return pltpu.make_async_copy(
            ids.at[s, pl.ds(vol_count * per_block, 1)], starts.at[pl.ds(s, 1)], start_sem.at[s]
        )

    local_ids.wait()
    start_copy(mine).start()

    def take_ids(k, unused):
        ids_copy(k).wait_recv()
        start_copy(sender(k)).start()
        return unused

    lax.fori_loop(1, near_count, take_ids, 0)

    def take_starts(s, unused):
        start_copy(s).wait()
        return unused

    lax.fori_loop(0, near_count, take_starts, 0)

    lane = iota((1, LANES), 1) // cols
    row = iota((bucket, LANES), 0)
    tile = iota((group_tiles, bucket), 0)

    def unpack(q, s):
        value = arrived[q, s]
        rolled = [value] + [pltpu.roll(value, d * cols, 1) for d in range(1, half)]
        for u in range(half):
            spread = rolled[(half - u) % half]
            for v in range(1, half):
                spread = jnp.where(wide == v, rolled[(v - u) % half], spread)
            first = pl.multiple_of(q * bucket + u * sub, sub)
            rows_ref[s, pl.ds(first, sub), :] = spread

    def accumulate(b, senders):
        places, values = [], []
        for s in senders:
            first = starts[s, b * half]
            low, high = jnp.zeros((1, LANES), I32), jnp.full((1, LANES), bucket, I32)
            for u in range(1, half):
                bound = starts[s, b * half + u] - first
                low = jnp.where(lane == u, bound, low)
                high = jnp.where(lane == u - 1, bound, high)
            keep = (row >= low) & (row < high)
            values.append(halves(jnp.where(keep, rows_ref[s, pl.ds(first, bucket), :], 0.0)))
            names = jnp.concatenate(
                [ids[s, pl.ds(b * per_block + j, 1), :] for j in range(per_block)], axis=1
            )
            places.append(onehot(tile == names))
        acc[...] += dot(jnp.concatenate(places, axis=1), jnp.concatenate(values, axis=0))

    def swap_copy(b, k):
        other = (member + k) % members
        return pltpu.make_async_remote_copy(
            src_ref=partial.at[b, pl.ds(other * share, share)], dst_ref=swapped.at[b, k - 1],
            send_sem=swap_send.at[b, k], recv_sem=swap_recv.at[b, k],
            device_id=(vol, pix_of(other // 2, channel, other % 2)), device_id_type=MESH,
        )

    def swap(b):
        partial[b] = acc[:, :LANES] + acc[:, LANES:]
        for k in range(1, members):
            swap_copy(b, k).start()

    def reduced(b):
        for k in range(1, members):
            swap_copy(b, k).wait_recv()
        value = partial[b, pl.ds(pl.multiple_of(member * share, share), share), :]
        for k in range(1, members):
            value = value + swapped[b, k - 1]
        return value

    pieces = mid_send.shape[1]
    piece_rows = share // pieces

    def part(p):
        return pl.ds(p * piece_rows, piece_rows)

    def mid_copy(b, p):
        return pltpu.make_async_remote_copy(
            src_ref=sums.at[b, part(p)], dst_ref=crossed.at[b, part(p)],
            send_sem=mid_send.at[b, p], recv_sem=mid_recv.at[b, p],
            device_id=(across, pix), device_id_type=MESH,
        )

    def far(q, unused):
        acc[...] = jnp.zeros(acc.shape, F32)

        def one(p, unused):
            @pl.when(p == 0)
            def _():
                local_rows(q).wait()

            @pl.when(p > 0)
            def _():
                rows_copy(q, 2 * p).wait_recv()

            rows_copy(q, 2 * p + 1).wait_recv()
            senders = [sender(2 * p), sender(2 * p + 1)]
            for s in senders:
                unpack(q, s)
            accumulate(q, senders)
            return unused

        lax.fori_loop(0, half, one, 0)
        swap(q)
        sums[q] = reduced(q)
        for p in range(pieces):
            mid_copy(q, p).start()
        return unused

    lax.fori_loop(0, half, far, 0)

    def off(i):
        return (i + half - place) % half

    def far_copy(i, k, p):
        return pltpu.make_async_remote_copy(
            src_ref=total.at[i, part(p)], dst_ref=gathered.at[core, place, chip, part(p)],
            send_sem=far_send.at[off(i), k, p], recv_sem=far_recv.at[off(i), k, p],
            device_id=(side * half + i, (chip + k) % chips * 2 + core), device_id_type=MESH,
        )

    def own_copy():
        return pltpu.make_async_copy(total.at[place], gathered.at[core, place, chip], own_sem)

    def finalize(i):
        value = reduced(half + i)
        for p in range(pieces):
            mid_copy(i, p).wait_recv()
            rows = slice(p * piece_rows, (p + 1) * piece_rows)
            total[i, rows, :] = value[rows] + crossed[i, rows, :]

            @pl.when(i != place)
            def _():
                far_copy(i, 0, p).start()

            for k in range(1, chips):
                far_copy(i, k, p).start()

        @pl.when(i == place)
        def _():
            own_copy().start()

    def near(i, unused):
        acc[...] = jnp.zeros(acc.shape, F32)

        def some(p, unused):
            accumulate(half + i, [4 * p + j for j in range(4)])
            return unused

        lax.fori_loop(0, near_count // 4, some, 0)
        swap(half + i)

        @pl.when(i > 0)
        def _():
            finalize(i - 1)

        return unused

    lax.fori_loop(0, half, near, 0)
    finalize(half - 1)

    def pass_copy(o, k, p):
        piece = gathered.at[
            core, (place + half - o) % half, (chip + chips - k) % chips, part(p)
        ]
        return pltpu.make_async_remote_copy(
            src_ref=piece, dst_ref=piece,
            send_sem=pass_send.at[o, k, p], recv_sem=pass_recv.at[o, k, p],
            device_id=sibling, device_id_type=MESH,
        )

    def far_arrival(o, k, p):
        return pltpu.make_async_remote_copy(
            src_ref=total.at[0, part(p)], dst_ref=gathered.at[core, place, chip, part(p)],
            send_sem=far_send.at[o, k, p], recv_sem=far_recv.at[o, k, p],
            device_id=(side * half + (place + o) % half, (chip + k) % chips * 2 + core),
            device_id_type=MESH,
        )

    own_copy().wait()
    for p in range(pieces):
        pass_copy(0, 0, p).start()
    for p in range(pieces):
        for k in range(1, chips):
            far_arrival(0, k, p).wait_recv()
            pass_copy(0, k, p).start()

        def relay(o, unused):
            for k in range(chips):
                far_arrival(o, k, p).wait_recv()
                pass_copy(o, k, p).start()
            return unused

        lax.fori_loop(1, half, relay, 0)

    def passed(o, unused):
        for k in range(chips):
            for p in range(pieces):
                pass_copy(o, k, p).wait()
        return unused

    lax.fori_loop(0, half, passed, 0)

    def sent(o, unused):
        for p in range(pieces):
            @pl.when(o > 0)
            def _():
                far_arrival(o, 0, p).wait_send()

            for k in range(1, chips):
                far_arrival(o, k, p).wait_send()
        return unused

    lax.fori_loop(0, half, sent, 0)

    def sent_rows(k, unused):
        ids_copy(k).wait_send()

        def one(q, unused):
            rows_copy(q, k).wait_send()
            return unused

        lax.fori_loop(0, half, one, 0)
        return unused

    lax.fori_loop(1, near_count, sent_rows, 0)

    def sent_sums(b, unused):
        for p in range(pieces):
            mid_copy(b, p).wait_send()
        for k in range(1, members):
            swap_copy(b, k).wait_send()
            swap_copy(half + b, k).wait_send()
        return unused

    lax.fori_loop(0, half, sent_sums, 0)


def finish(
    gathered, rank_ref, owned_hbm, shell_hbm, split_ref, shell_ref, owned_ref, shell_sem, owned_sem,
):
    half, chips, share = gathered.shape[1], gathered.shape[2], gathered.shape[3]
    cols = LANES // half
    owned_most = owned_ref.shape[0]
    block_tiles = shell_ref.shape[0]
    group_tiles = block_tiles // half
    lane = iota((share, LANES), 1) // cols
    for core in range(2):
        for chip in range(chips):
            first, channel = (chip // 2 * 2 + core) * share, chip % 2
            values = turn_groups([gathered[core, s, chip] for s in range(half)], lane, cols)
            for u in range(half):
                value = values[u]
                start = u * group_tiles + first
                shell_ref[start:start + share, channel * LANES:(channel + 1) * LANES] = value
                both = halves(value)
                for part in range(2):
                    at = (2 * part + channel) * LANES
                    split_ref[start:start + share, at:at + LANES] = both[:, part * LANES:(part + 1) * LANES]
    shell_copy = pltpu.make_async_copy(shell_ref, shell_hbm, shell_sem)
    shell_copy.start()
    rank = jnp.concatenate([rank_ref[q:q + 1, :] for q in range(rank_ref.shape[0])], axis=1)
    moved = dot(onehot(iota((owned_most, block_tiles), 0) == rank), split_ref[...])
    owned_ref[...] = moved[:, :2 * LANES] + moved[:, 2 * LANES:]
    owned_copy = pltpu.make_async_copy(owned_ref, owned_hbm, owned_sem)
    owned_copy.start()
    shell_copy.wait()
    owned_copy.wait()


def shards(kernel, pressure, velocity, entry_slot, slot_tile, tile_owner):
    vol_count, pix_count = lax.axis_size("vol"), lax.axis_size("pix")
    device_count = vol_count * pix_count
    entries = kernel.shape[0]
    slots = slot_tile.shape[1]
    tiles = tile_owner.shape[0]
    block_tiles = tiles // vol_count
    owned_most = 2 * block_tiles // pix_count
    bucket = 2 * slots // vol_count
    width = 2 * kernel.shape[1]
    vmem = pl.BlockSpec(memory_space=pltpu.VMEM)
    anywhere = pl.BlockSpec(memory_space=pl.ANY)
    hbm = pl.BlockSpec(memory_space=pltpu.HBM)
    dma = pltpu.SemaphoreType.DMA

    shape = (entries // LANES, LANES)
    half = vol_count // 2
    sub = bucket // half
    id_rows = vol_count * bucket // LANES + 8
    split, place, ids, rank = pl.pallas_call(
        functools.partial(prepare, (vol_count, pix_count, slots, block_tiles, bucket)),
        out_shape=(
            jax.ShapeDtypeStruct((slots, 2 * width), BF16),
            jax.ShapeDtypeStruct((1, slots), I32),
            jax.ShapeDtypeStruct((id_rows, LANES), I32),
            jax.ShapeDtypeStruct((block_tiles // LANES, LANES), I32),
        ),
        in_specs=[hbm] * 6,
        out_specs=(vmem, vmem, vmem, vmem),
        scratch_shapes=[
            pltpu.VMEM(kernel.shape, BF16),
            pltpu.SMEM(shape, I32),
            pltpu.VMEM(shape, BF16),
            pltpu.VMEM(shape, BF16),
            pltpu.VMEM(shape, I32),
            pltpu.VMEM((1, slots), I32),
            pltpu.VMEM((block_tiles // LANES, LANES), I32),
            pltpu.VMEM(shape, F32),
            pltpu.VMEM(shape, F32),
            pltpu.VMEM((slots + WINDOW, width), F32),
            dma((4,)),
            dma((6,)),
        ],
        compiler_params=pltpu.CompilerParams(vmem_limit_bytes=PREPARE_VMEM),
        name="prepare",
    )(*[
        pltpu.with_memory_space_constraint(x, pltpu.HBM) for x in (
            kernel, pressure.reshape(shape), velocity.reshape(shape), entry_slot.reshape(shape),
            slot_tile, tile_owner.reshape(tiles // LANES, LANES),
        )
    ])

    chips = pix_count // 2
    near, pieces = vol_count, 1
    group_tiles = block_tiles // half
    share = group_tiles // chips
    gathered = pl.pallas_call(
        functools.partial(exchange, (vol_count, pix_count, block_tiles, bucket)),
        out_shape=jax.ShapeDtypeStruct((2, half, chips, share, LANES), F32),
        in_specs=[vmem, vmem, anywhere],
        out_specs=vmem,
        scratch_shapes=[
            pltpu.VMEM((half, 2, half, sub, LANES), F32),
            pltpu.VMEM((half, near, sub, LANES), F32),
            pltpu.VMEM((near, id_rows, LANES), I32),
            pltpu.SMEM((near, LANES), I32),
            pltpu.VMEM((near, (half + 1) * bucket, LANES), F32),
            pltpu.VMEM((group_tiles, 2 * LANES), F32),
            pltpu.VMEM((vol_count, group_tiles, LANES), F32),
            pltpu.VMEM((vol_count, chips - 1, share, LANES), F32),
            pltpu.VMEM((half, share, LANES), F32),
            pltpu.VMEM((half, share, LANES), F32),
            pltpu.VMEM((half, share, LANES), F32),
            dma((half, near)), dma((half, near)), dma((near,)), dma((near,)),
            dma((half + 1,)), dma((near,)), dma((vol_count, chips)), dma((vol_count, chips)),
            dma((half, pieces)), dma((half, pieces)), dma((half, chips, pieces)),
            dma((half, chips, pieces)), dma, dma((half, chips, pieces)), dma((half, chips, pieces)),
        ],
        compiler_params=pltpu.CompilerParams(
            collective_id=0, has_side_effects=True, vmem_limit_bytes=EXCHANGE_VMEM
        ),
        name="exchange",
    )(split, place, ids)

    return pl.pallas_call(
        finish,
        out_shape=(
            jax.ShapeDtypeStruct((owned_most, width), F32),
            jax.ShapeDtypeStruct((block_tiles, width), F32),
        ),
        in_specs=[vmem, vmem],
        out_specs=(anywhere, anywhere),
        scratch_shapes=[
            pltpu.VMEM((block_tiles, 2 * width), BF16),
            pltpu.VMEM((block_tiles, width), F32),
            pltpu.VMEM((owned_most, width), F32),
            dma,
            dma,
        ],
        compiler_params=pltpu.CompilerParams(vmem_limit_bytes=FINISH_VMEM),
        name="finish",
    )(gathered, rank)


def solution(mesh):
    in_specs = (
        P(("vol", "pix"), None),
        P(("vol", "pix")),
        P(("vol", "pix")),
        P(("vol", "pix"), None),
        P(("vol", "pix"), None),
        P(),
    )
    out_specs = (P(("vol", "pix"), None), P("vol", None))
    return jax.shard_map(shards, mesh=mesh, in_specs=in_specs, out_specs=out_specs, check_vma=False)
```

```python
import functools

import jax
import jax.numpy as jnp
from jax import lax
from jax.experimental import pallas as pl
from jax.experimental.pallas import tpu as pltpu
from jax.sharding import PartitionSpec as P

MESH = pl.DeviceIdType.MESH
LANES = 128
BLOCK = 256
WINDOW = 40
F32 = jnp.float32
BF16 = jnp.bfloat16
I32 = jnp.int32
PREPARE_VMEM = 24 << 20
EXCHANGE_VMEM = 24 << 20
FINISH_VMEM = 16 << 20


def iota(shape, axis):
    return lax.broadcasted_iota(I32, shape, axis)


def onehot(mask):
    return jnp.where(mask, 1.0, 0.0).astype(BF16)


def dot(a, b):
    return jnp.dot(a, b, preferred_element_type=F32)


def halves(x):
    high = x.astype(BF16)
    low = (x - high.astype(F32)).astype(BF16)
    return jnp.concatenate([high, low], axis=1)


def turn_groups(values, lane, cols):
    values = list(values)
    step = 1
    while step < len(values):
        upper = lane // step % 2 == 1
        for i in range(len(values)):
            if i // step % 2 == 0:
                a, b = values[i], values[i + step]
                values[i] = jnp.where(upper, pltpu.roll(b, step * cols, 1), a)
                values[i + step] = jnp.where(upper, b, pltpu.roll(a, LANES - step * cols, 1))
        step *= 2
    return values


def prepare(
    dims, kern_hbm, thermal_hbm, kinetic_hbm, slot_hbm, tile_hbm, owner_hbm,
    split_ref, place_ref, ids_ref, rank_ref, kern_ref, slot_smem, thermal_ref, kinetic_ref, slot_ref,
    tile_ref, owner_ref, thermal32, kinetic32, part_ref, sems, small_sem,
):
    vol_count, pix_count, slots, block_tiles, bucket = dims
    entries = kern_ref.shape[0]
    blocks = entries // BLOCK
    pieces = sems.shape[0]
    piece = entries // pieces
    lines = BLOCK // LANES

    block_high = block_tiles // LANES
    first_high = pl.multiple_of(lax.axis_index("vol") * block_high, block_high)
    small = [
        pltpu.make_async_copy(tile_hbm, tile_ref, small_sem.at[0]),
        pltpu.make_async_copy(owner_hbm.at[pl.ds(first_high, block_high)], owner_ref, small_sem.at[1]),
        pltpu.make_async_copy(slot_hbm, slot_smem, small_sem.at[2]),
        pltpu.make_async_copy(slot_hbm, slot_ref, small_sem.at[3]),
        pltpu.make_async_copy(thermal_hbm, thermal_ref, small_sem.at[4]),
        pltpu.make_async_copy(kinetic_hbm, kinetic_ref, small_sem.at[5]),
    ]
    for copy in small:
        copy.start()

    def fetch(q):
        rows = pl.ds(q * piece, piece)
        return pltpu.make_async_copy(kern_hbm.at[rows], kern_ref.at[rows], sems.at[q])

    for q in range(pieces):
        fetch(q).start()

    small[0].wait()
    small[1].wait()
    mine = owner_ref[...] == lax.axis_index("pix")
    ones = jnp.where(mine, 1.0, 0.0)
    upper = onehot(iota((LANES, LANES), 0) < iota((LANES, LANES), 1))
    above = onehot(iota((block_high, block_high), 1) < iota((block_high, block_high), 0))
    total = jnp.broadcast_to(jnp.sum(ones, axis=1, keepdims=True), (block_high, LANES))
    rank = dot(ones.astype(BF16), upper) + dot(above, total.astype(BF16))
    rank_ref[...] = jnp.where(mine, rank, -1.0).astype(I32)

    half = vol_count // 2
    side = lax.axis_index("vol") // half
    tile = tile_ref[...]
    block, low = tile // block_tiles, tile % block_tiles
    order = (block + vol_count - (1 - side) * half) % vol_count
    group_tiles = block_tiles // half
    kinds = vol_count * half
    to_kind = iota((kinds, slots), 0) == order * half + low // group_tiles
    ones = jnp.where(to_kind, 1.0, 0.0)
    carry = jnp.zeros((kinds, 1), F32)
    position = []
    for j in range(slots // LANES):
        chunk = ones[:, j * LANES:(j + 1) * LANES]
        ranks = dot(chunk.astype(BF16), upper) + carry
        position.append(jnp.sum(chunk * ranks, axis=0, keepdims=True))
        carry = carry + jnp.sum(chunk, axis=1, keepdims=True)
    counts = jnp.broadcast_to(carry, (kinds, LANES)).astype(BF16)
    earlier = iota((kinds, kinds), 1) < iota((kinds, kinds), 0)
    same = iota((kinds, kinds), 1) // half == iota((kinds, kinds), 0) // half
    starts = dot(onehot(earlier), counts)
    inner = dot(onehot(earlier & same), counts)
    position = jnp.concatenate(position, axis=1)
    place_ref[...] = (position + jnp.sum(ones * starts[:, 0:1], axis=0, keepdims=True)).astype(I32)
    position = (position + jnp.sum(ones * inner[:, 0:1], axis=0, keepdims=True)).astype(I32)

    places = onehot(iota((bucket, slots), 0) == position)
    to_block = iota((vol_count, slots), 0) == order
    values = jnp.where(to_block, (low % group_tiles + 1).astype(F32), 0.0)
    rows = lax.dot_general(
        values.astype(BF16), places, (((1,), (1,)), ((), ())), preferred_element_type=F32
    )
    rows = (rows - 1.0).astype(I32)
    per_block = bucket // LANES
    names = jnp.concatenate(
        [rows[b:b + 1, q * LANES:(q + 1) * LANES] for b in range(vol_count) for q in range(per_block)],
        axis=0,
    )
    ids_ref[0:vol_count * per_block, :] = names
    on_lane = iota((kinds, LANES), 0) == iota((kinds, LANES), 1)
    line = jnp.sum(jnp.where(on_lane, starts, 0.0), axis=0, keepdims=True).astype(I32)
    ids_ref[vol_count * per_block:, :] = jnp.broadcast_to(line, (8, LANES))

    part_ref[...] = jnp.zeros_like(part_ref)
    within = iota((WINDOW, BLOCK), 0)
    for copy in small[2:]:
        copy.wait()
    thermal32[...] = thermal_ref[...].astype(F32)
    kinetic32[...] = kinetic_ref[...].astype(F32)

    def base_of(i):
        return slot_smem[lines * i, 0] // 8 * 8

    def add_window(i, base):
        def pair(ref):
            return jnp.concatenate([ref[pl.ds(lines * i + j, 1), :] for j in range(lines)], axis=1)

        base = pl.multiple_of(base, 8)
        match = within + base == pair(slot_ref)
        weights = jnp.concatenate(
            [jnp.where(match, pair(thermal32), 0.0), jnp.where(match, pair(kinetic32), 0.0)], axis=0
        ).astype(BF16)
        sums = dot(weights, kern_ref[pl.ds(pl.multiple_of(i * BLOCK, BLOCK), BLOCK), :])
        part_ref[pl.ds(base, WINDOW), 0:LANES] += sums[:WINDOW]
        part_ref[pl.ds(base, WINDOW), LANES:2 * LANES] += sums[WINDOW:]

    per = blocks // pieces
    for q in range(pieces):
        fetch(q).wait()

        def first_window(i, unused):
            add_window(i, base_of(i))
            return unused

        lax.fori_loop(q * per, (q + 1) * per, first_window, 0, unroll=32)

    def more_windows(i, unused):
        base = base_of(i)
        extra = (slot_smem[lines * i + lines - 1, LANES - 1] - base) // WINDOW

        def one(w, unused):
            add_window(i, base + w * WINDOW)
            return unused

        return lax.fori_loop(1, extra + 1, one, unused)

    rows = slot_ref.shape[0] - lines + 1
    ends = pltpu.roll(slot_ref[lines - 1:, :], 1, 1)
    spans = ends - slot_ref[0:rows, :] // 8 * 8
    first = (iota((rows, LANES), 1) == 0) & (iota((rows, LANES), 0) % lines == 0)

    @pl.when(jnp.max(jnp.where(first, spans, 0)) >= WINDOW)
    def _():
        lax.fori_loop(0, blocks, more_windows, 0)

    split_ref[...] = halves(part_ref[0:slots, :])


def exchange(
    dims, split_ref, place_ref, ids_hbm, gathered, out_ref, arrived, ids, starts, rows_ref, acc, partial, swapped, sums,
    crossed, total, send_sem, recv_sem, ids_send, ids_recv, local_sem, start_sem, swap_send,
    swap_recv, mid_send, mid_recv, far_send, far_recv, own_sem, pass_send, pass_recv,
):
    vol_count, pix_count, block_tiles, bucket = dims
    half = vol_count // 2
    near_count = 2 * half
    chips = pix_count // 2
    members = chips
    cols, sub = LANES // half, bucket // half
    group_tiles = block_tiles // half
    share = group_tiles // members
    per_block = bucket // LANES
    vol, pix = lax.axis_index("vol"), lax.axis_index("pix")
    side, place = vol // half, vol % half
    chip, core = pix // 2, pix % 2
    group, channel = chip // 2, chip % 2
    member = group * 2 + core
    across = (vol + half) % vol_count
    mine = place * 2 + channel
    sibling = (vol, pix - core + (1 - core))
    id_rows = vol_count * per_block + 1

    def peer(k):
        return (place + k // 2) % half, (channel + k % 2) % 2

    def sender(k):
        return (place + half - k // 2) % half * 2 + (channel + k % 2) % 2

    def pix_of(other_group, other_channel, other_core):
        return (other_group * 2 + other_channel) * 2 + other_core

    barrier = pltpu.get_barrier_semaphore()

    def signal(other_vol, other_pix):
        pl.semaphore_signal(
            barrier, inc=1, device_id=(other_vol, other_pix), device_id_type=MESH
        )

    def greet(k, unused):
        signal(side * half + (place + k // chips) % half, (chip + k % chips) % chips * 2 + core)
        return unused

    signal(across, pix)
    for k in range(1, pix_count):
        signal(vol, (pix + k) % pix_count)
    lax.fori_loop(chips, half * chips, greet, 0)

    wide = iota((sub, LANES), 1) // cols
    slots = place_ref.shape[1]

    def permute(q):
        moved = dot(onehot(iota((bucket, slots), 0) + q * bucket == place_ref[...]), split_ref[...])
        for c in range(2):
            high, low = c * LANES, (c + 2) * LANES
            value = moved[:, high:high + LANES] + moved[:, low:low + LANES]
            parts = [value[u * sub:(u + 1) * sub] for u in range(half)]
            for h, packed in enumerate(turn_groups(parts, wide, cols)):
                out_ref[h, c, q] = packed

    permute(0)
    pl.semaphore_wait(barrier, pix_count + (half - 1) * chips)

    def target(k):
        other_place, other_channel = peer(k)
        return side * half + other_place, pix_of(group, other_channel, core)

    def rows_copy(q, k):
        other_place, other_channel = peer(k)
        return pltpu.make_async_remote_copy(
            src_ref=out_ref.at[other_place, other_channel, q], dst_ref=arrived.at[q, mine],
            send_sem=send_sem.at[q, k], recv_sem=recv_sem.at[q, k],
            device_id=target(k), device_id_type=MESH,
        )

    def ids_copy(k):
        return pltpu.make_async_remote_copy(
            src_ref=ids_hbm.at[pl.ds(0, id_rows)], dst_ref=ids.at[mine, pl.ds(0, id_rows)],
            send_sem=ids_send.at[k], recv_sem=ids_recv.at[k],
            device_id=target(k), device_id_type=MESH,
        )

    def local_rows(q):
        return pltpu.make_async_copy(
            out_ref.at[place, channel, q], arrived.at[q, mine], local_sem.at[q]
        )

    local_ids = pltpu.make_async_copy(ids_hbm, ids.at[mine], local_sem.at[half])

    def send_ids(k, unused):
        ids_copy(k).start()
        return unused

    lax.fori_loop(1, near_count, send_ids, 0)
    local_ids.start()

    def send_chunk(q, unused):
        @pl.when(q > 0)
        def _():
            permute(q)

        def one(k, unused):
            rows_copy(q, k).start()
            return unused

        lax.fori_loop(1, near_count, one, 0)
        local_rows(q).start()
        return unused

    lax.fori_loop(0, half, send_chunk, 0)

    def clear(s, unused):
        rows_ref[s, half * bucket:(half + 1) * bucket, :] = jnp.zeros((bucket, LANES), F32)
        return unused

    lax.fori_loop(0, near_count, clear, 0)

    def start_copy(s):
        return pltpu.make_async_copy(
            ids.at[s, pl.ds(vol_count * per_block, 1)], starts.at[pl.ds(s, 1)], start_sem.at[s]
        )

    local_ids.wait()
    start_copy(mine).start()

    def take_ids(k, unused):
        ids_copy(k).wait_recv()
        start_copy(sender(k)).start()
        return unused

    lax.fori_loop(1, near_count, take_ids, 0)

    def take_starts(s, unused):
        start_copy(s).wait()
        return unused

    lax.fori_loop(0, near_count, take_starts, 0)

    lane = iota((1, LANES), 1) // cols
    row = iota((bucket, LANES), 0)
    tile = iota((group_tiles, bucket), 0)

    def unpack(q, s):
        value = arrived[q, s]
        rolled = [value] + [pltpu.roll(value, d * cols, 1) for d in range(1, half)]
        for u in range(half):
            spread = rolled[(half - u) % half]
            for v in range(1, half):
                spread = jnp.where(wide == v, rolled[(v - u) % half], spread)
            first = pl.multiple_of(q * bucket + u * sub, sub)
            rows_ref[s, pl.ds(first, sub), :] = spread

    def accumulate(b, senders):
        places, values = [], []
        for s in senders:
            first = starts[s, b * half]
            low, high = jnp.zeros((1, LANES), I32), jnp.full((1, LANES), bucket, I32)
            for u in range(1, half):
                bound = starts[s, b * half + u] - first
                low = jnp.where(lane == u, bound, low)
                high = jnp.where(lane == u - 1, bound, high)
            keep = (row >= low) & (row < high)
            values.append(halves(jnp.where(keep, rows_ref[s, pl.ds(first, bucket), :], 0.0)))
            names = jnp.concatenate(
                [ids[s, pl.ds(b * per_block + j, 1), :] for j in range(per_block)], axis=1
            )
            places.append(onehot(tile == names))
        acc[...] += dot(jnp.concatenate(places, axis=1), jnp.concatenate(values, axis=0))

    def swap_copy(b, k):
        other = (member + k) % members
        return pltpu.make_async_remote_copy(
            src_ref=partial.at[b, pl.ds(other * share, share)], dst_ref=swapped.at[b, k - 1],
            send_sem=swap_send.at[b, k], recv_sem=swap_recv.at[b, k],
            device_id=(vol, pix_of(other // 2, channel, other % 2)), device_id_type=MESH,
        )

    def swap(b):
        partial[b] = acc[:, :LANES] + acc[:, LANES:]
        for k in range(1, members):
            swap_copy(b, k).start()

    def reduced(b):
        for k in range(1, members):
            swap_copy(b, k).wait_recv()
        value = partial[b, pl.ds(pl.multiple_of(member * share, share), share), :]
        for k in range(1, members):
            value = value + swapped[b, k - 1]
        return value

    pieces = mid_send.shape[1]
    piece_rows = share // pieces

    def part(p):
        return pl.ds(p * piece_rows, piece_rows)

    def mid_copy(b, p):
        return pltpu.make_async_remote_copy(
            src_ref=sums.at[b, part(p)], dst_ref=crossed.at[b, part(p)],
            send_sem=mid_send.at[b, p], recv_sem=mid_recv.at[b, p],
            device_id=(across, pix), device_id_type=MESH,
        )

    def far_sum(q):
        acc[...] = jnp.zeros(acc.shape, F32)

        def one(p, unused):
            @pl.when(p == 0)
            def _():
                local_rows(q).wait()

            @pl.when(p > 0)
            def _():
                rows_copy(q, 2 * p).wait_recv()

            rows_copy(q, 2 * p + 1).wait_recv()
            senders = [sender(2 * p), sender(2 * p + 1)]
            for s in senders:
                unpack(q, s)
            accumulate(q, senders)
            return unused

        lax.fori_loop(0, half, one, 0)
        swap(q)

    def near_sum(i, unused):
        acc[...] = jnp.zeros(acc.shape, F32)

        def some(p, unused):
            accumulate(half + i, [4 * p + j for j in range(4)])
            return unused

        lax.fori_loop(0, near_count // 4, some, 0)
        swap(half + i)
        return unused

    def send_far(q):
        sums[q] = reduced(q)
        for p in range(pieces):
            mid_copy(q, p).start()

    def far(q, unused):
        far_sum(q)

        @pl.when(q > 0)
        def _():
            send_far(q - 1)

        return unused

    lax.fori_loop(0, half, far, 0)

    def off(i):
        return (i + half - place) % half

    def far_copy(i, k, p):
        return pltpu.make_async_remote_copy(
            src_ref=total.at[i, part(p)], dst_ref=gathered.at[core, place, chip, part(p)],
            send_sem=far_send.at[off(i), k, p], recv_sem=far_recv.at[off(i), k, p],
            device_id=(side * half + i, (chip + k) % chips * 2 + core), device_id_type=MESH,
        )

    def own_copy():
        return pltpu.make_async_copy(total.at[place], gathered.at[core, place, chip], own_sem)

    def finalize(i):
        value = reduced(half + i)
        for p in range(pieces):
            mid_copy(i, p).wait_recv()
            rows = slice(p * piece_rows, (p + 1) * piece_rows)
            total[i, rows, :] = value[rows] + crossed[i, rows, :]

            @pl.when(i != place)
            def _():
                far_copy(i, 0, p).start()

            for k in range(1, chips):
                far_copy(i, k, p).start()

        @pl.when(i == place)
        def _():
            own_copy().start()

    early = 2
    lax.fori_loop(0, early, near_sum, 0)
    send_far(half - 1)

    def finish_near(i, unused):
        near_sum(i, 0)
        finalize(i - 1)
        return unused

    def finish_last(i, unused):
        finalize(i)
        return unused

    finalize(0)
    lax.fori_loop(early, half, finish_near, 0)
    lax.fori_loop(half - 1, half, finish_last, 0)

    def pass_copy(o, k, p):
        piece = gathered.at[
            core, (place + half - o) % half, (chip + chips - k) % chips, part(p)
        ]
        return pltpu.make_async_remote_copy(
            src_ref=piece, dst_ref=piece,
            send_sem=pass_send.at[o, k, p], recv_sem=pass_recv.at[o, k, p],
            device_id=sibling, device_id_type=MESH,
        )

    def far_arrival(o, k, p):
        return pltpu.make_async_remote_copy(
            src_ref=total.at[0, part(p)], dst_ref=gathered.at[core, place, chip, part(p)],
            send_sem=far_send.at[o, k, p], recv_sem=far_recv.at[o, k, p],
            device_id=(side * half + (place + o) % half, (chip + k) % chips * 2 + core),
            device_id_type=MESH,
        )

    own_copy().wait()
    for p in range(pieces):
        pass_copy(0, 0, p).start()
    for p in range(pieces):
        for k in range(1, chips):
            far_arrival(0, k, p).wait_recv()
            pass_copy(0, k, p).start()

        def relay(o, unused):
            for k in range(chips):
                far_arrival(o, k, p).wait_recv()
                pass_copy(o, k, p).start()
            return unused

        lax.fori_loop(1, half, relay, 0)

    def passed(o, unused):
        for k in range(chips):
            for p in range(pieces):
                pass_copy(o, k, p).wait()
        return unused

    lax.fori_loop(0, half, passed, 0)

    def sent(o, unused):
        for p in range(pieces):
            @pl.when(o > 0)
            def _():
                far_arrival(o, 0, p).wait_send()

            for k in range(1, chips):
                far_arrival(o, k, p).wait_send()
        return unused

    lax.fori_loop(0, half, sent, 0)

    def sent_rows(k, unused):
        ids_copy(k).wait_send()

        def one(q, unused):
            rows_copy(q, k).wait_send()
            return unused

        lax.fori_loop(0, half, one, 0)
        return unused

    lax.fori_loop(1, near_count, sent_rows, 0)

    def sent_sums(b, unused):
        for p in range(pieces):
            mid_copy(b, p).wait_send()
        for k in range(1, members):
            swap_copy(b, k).wait_send()
            swap_copy(half + b, k).wait_send()
        return unused

    lax.fori_loop(0, half, sent_sums, 0)


def finish(
    gathered, rank_ref, owned_hbm, shell_hbm, split_ref, shell_ref, owned_ref, shell_sem, owned_sem,
):
    half, chips, share = gathered.shape[1], gathered.shape[2], gathered.shape[3]
    cols = LANES // half
    owned_most = owned_ref.shape[0]
    block_tiles = shell_ref.shape[0]
    group_tiles = block_tiles // half
    lane = iota((share, LANES), 1) // cols
    for core in range(2):
        for chip in range(chips):
            first, channel = (chip // 2 * 2 + core) * share, chip % 2
            values = turn_groups([gathered[core, s, chip] for s in range(half)], lane, cols)
            for u in range(half):
                value = values[u]
                start = u * group_tiles + first
                shell_ref[start:start + share, channel * LANES:(channel + 1) * LANES] = value
                both = halves(value)
                for part in range(2):
                    at = (2 * part + channel) * LANES
                    split_ref[start:start + share, at:at + LANES] = both[:, part * LANES:(part + 1) * LANES]
    shell_copy = pltpu.make_async_copy(shell_ref, shell_hbm, shell_sem)
    shell_copy.start()
    rank = jnp.concatenate([rank_ref[q:q + 1, :] for q in range(rank_ref.shape[0])], axis=1)
    moved = dot(onehot(iota((owned_most, block_tiles), 0) == rank), split_ref[...])
    owned_ref[...] = moved[:, :2 * LANES] + moved[:, 2 * LANES:]
    owned_copy = pltpu.make_async_copy(owned_ref, owned_hbm, owned_sem)
    owned_copy.start()
    shell_copy.wait()
    owned_copy.wait()


def shards(kernel, pressure, velocity, entry_slot, slot_tile, tile_owner):
    vol_count, pix_count = lax.axis_size("vol"), lax.axis_size("pix")
    device_count = vol_count * pix_count
    entries = kernel.shape[0]
    slots = slot_tile.shape[1]
    tiles = tile_owner.shape[0]
    block_tiles = tiles // vol_count
    owned_most = 2 * block_tiles // pix_count
    bucket = 2 * slots // vol_count
    width = 2 * kernel.shape[1]
    vmem = pl.BlockSpec(memory_space=pltpu.VMEM)
    anywhere = pl.BlockSpec(memory_space=pl.ANY)
    hbm = pl.BlockSpec(memory_space=pltpu.HBM)
    dma = pltpu.SemaphoreType.DMA

    shape = (entries // LANES, LANES)
    half = vol_count // 2
    sub = bucket // half
    id_rows = vol_count * bucket // LANES + 8
    split, place, ids, rank = pl.pallas_call(
        functools.partial(prepare, (vol_count, pix_count, slots, block_tiles, bucket)),
        out_shape=(
            jax.ShapeDtypeStruct((slots, 2 * width), BF16),
            jax.ShapeDtypeStruct((1, slots), I32),
            jax.ShapeDtypeStruct((id_rows, LANES), I32),
            jax.ShapeDtypeStruct((block_tiles // LANES, LANES), I32),
        ),
        in_specs=[hbm] * 6,
        out_specs=(vmem, vmem, vmem, vmem),
        scratch_shapes=[
            pltpu.VMEM(kernel.shape, BF16),
            pltpu.SMEM(shape, I32),
            pltpu.VMEM(shape, BF16),
            pltpu.VMEM(shape, BF16),
            pltpu.VMEM(shape, I32),
            pltpu.VMEM((1, slots), I32),
            pltpu.VMEM((block_tiles // LANES, LANES), I32),
            pltpu.VMEM(shape, F32),
            pltpu.VMEM(shape, F32),
            pltpu.VMEM((slots + WINDOW, width), F32),
            dma((2,)),
            dma((6,)),
        ],
        compiler_params=pltpu.CompilerParams(vmem_limit_bytes=PREPARE_VMEM),
        name="prepare",
    )(*[
        pltpu.with_memory_space_constraint(x, pltpu.HBM) for x in (
            kernel, pressure.reshape(shape), velocity.reshape(shape), entry_slot.reshape(shape),
            slot_tile, tile_owner.reshape(tiles // LANES, LANES),
        )
    ])

    chips = pix_count // 2
    near, pieces = vol_count, 1
    group_tiles = block_tiles // half
    share = group_tiles // chips
    gathered = pl.pallas_call(
        functools.partial(exchange, (vol_count, pix_count, block_tiles, bucket)),
        out_shape=jax.ShapeDtypeStruct((2, half, chips, share, LANES), F32),
        in_specs=[vmem, vmem, anywhere],
        out_specs=vmem,
        scratch_shapes=[
            pltpu.VMEM((half, 2, half, sub, LANES), F32),
            pltpu.VMEM((half, near, sub, LANES), F32),
            pltpu.VMEM((near, id_rows, LANES), I32),
            pltpu.SMEM((near, LANES), I32),
            pltpu.VMEM((near, (half + 1) * bucket, LANES), F32),
            pltpu.VMEM((group_tiles, 2 * LANES), F32),
            pltpu.VMEM((vol_count, group_tiles, LANES), F32),
            pltpu.VMEM((vol_count, chips - 1, share, LANES), F32),
            pltpu.VMEM((half, share, LANES), F32),
            pltpu.VMEM((half, share, LANES), F32),
            pltpu.VMEM((half, share, LANES), F32),
            dma((half, near)), dma((half, near)), dma((near,)), dma((near,)),
            dma((half + 1,)), dma((near,)), dma((vol_count, chips)), dma((vol_count, chips)),
            dma((half, pieces)), dma((half, pieces)), dma((half, chips, pieces)),
            dma((half, chips, pieces)), dma, dma((half, chips, pieces)), dma((half, chips, pieces)),
        ],
        compiler_params=pltpu.CompilerParams(
            collective_id=0, has_side_effects=True, vmem_limit_bytes=EXCHANGE_VMEM
        ),
        name="exchange",
    )(split, place, ids)

    return pl.pallas_call(
        finish,
        out_shape=(
            jax.ShapeDtypeStruct((owned_most, width), F32),
            jax.ShapeDtypeStruct((block_tiles, width), F32),
        ),
        in_specs=[vmem, vmem],
        out_specs=(anywhere, anywhere),
        scratch_shapes=[
            pltpu.VMEM((block_tiles, 2 * width), BF16),
            pltpu.VMEM((block_tiles, width), F32),
            pltpu.VMEM((owned_most, width), F32),
            dma,
            dma,
        ],
        compiler_params=pltpu.CompilerParams(vmem_limit_bytes=FINISH_VMEM),
        name="finish",
    )(gathered, rank)


def solution(mesh):
    in_specs = (
        P(("vol", "pix"), None),
        P(("vol", "pix")),
        P(("vol", "pix")),
        P(("vol", "pix"), None),
        P(("vol", "pix"), None),
        P(),
    )
    out_specs = (P(("vol", "pix"), None), P("vol", None))
    return jax.shard_map(shards, mesh=mesh, in_specs=in_specs, out_specs=out_specs, check_vma=False)
```
